128 devices in a mesh: leaf: 128 (over x, z, y, core).
Axes of the slice: x: 4, y: 4, z: 4, core: 2. Of those that a mesh axis runs over, the one named last changes fastest.
Arguments:
- slip: bfloat16 [128, 32768], P(None, 'leaf'), may hold values from -6 to 6
- to_multipole: bfloat16 [121, 128], replicated, may hold values from -0.5 to 0.5
- up_shift: float32 [2, 121, 121], replicated, may hold values from -0.375 to 0.375
- down_shift: float32 [2, 121, 121], replicated, may hold values from -0.5 to 0.5
- sibling_far: float32 [2, 121, 121], replicated, may hold values from -0.5 to 0.5
- leaf_far: bfloat16 [27, 121, 121], replicated, may hold values from -0.25 to 0.25
- to_stress: bfloat16 [128, 121], replicated, may hold values from -0.125 to 0.125
- near_blocks: bfloat16 [9, 128, 128], replicated, may hold values from -0.1875 to 0.1875
- send_cells: int32 [128, 16384], P('leaf'), may hold values from 0 to 255, as said below
- far_list: int32 [27, 32768], P(None, 'leaf'), may hold values from 0 to 16639, as said below
- near_list: int32 [9, 32768], P(None, 'leaf'), may hold values from 0 to 319, as said below
Outputs:
- stress: float32 [128, 32768], P(None, 'leaf')
The draws below stay inside these ranges and needn't reach their ends.
Inputs may be any that keep to these rules, and one draw needn't show every extreme that they name: `send_cells`: row q holds, in positions d * 128 to (d + 1) * 128 - 1, 128 distinct cells of device q (numbered within that device) listed for receiving device d. `far_list`: an entry v below 256 names a cell of the target's own device. Otherwise v - 256 = q * 128 + s names slot s of device q's list for the target's device, q is not the target's device, s < 128 when q lies within 4 devices of it and s < 32 when it lies farther; in every draw some entry names slot 127 of a device within 4, and some names slot 31 of a farther device. `near_list`: an entry w names the cell w - 32 counted from the first cell of the target's device, so that positions before 0 and from 256 on lie on the neighbouring devices (zeros outside the fault); entry 4 is the target itself.
All inputs are finite; a program needn't handle non-finite values.
Results may differ from the reference program's by a relative error of at most 0.0031.
Values may be sent and summed in bfloat16 or wider, within the bound.
No kernel may reach another device: no remote copies, remote signals or barrier semaphores. Data moves between devices by JAX's collectives and lax.ppermute only.
A program may use at most 64 MiB of HBM per device.

```python
import jax
import jax.numpy as jnp
from jax import lax

ELEM = 128
COEF = 121
NEAR = 9
TYPES = 27
NEAR_PEERS = 4
CELLS_DEV = 256
HALO = 32
CAP_NEAR = 128
CAP_FAR = 32
CELLS = 32768
N_LEAF = 128


def let_plan(key):
    base = jax.random.fold_in(key, 4127)
    keys = jax.random.split(base, 5)
    devices_all = N_LEAF
    receiver = jnp.arange(devices_all, dtype=jnp.int32)[:, None]
    sender = jnp.arange(devices_all, dtype=jnp.int32)[None, :]
    apart = jnp.abs(sender - receiver)
    close_count = jax.random.randint(keys[0], (devices_all, devices_all), CAP_NEAR // 4, CAP_NEAR + 1)
    far_count = jax.random.randint(keys[1], (devices_all, devices_all), CAP_FAR // 2, CAP_FAR + 1)
    counts = jnp.where(apart == 0, 0, jnp.where(apart <= NEAR_PEERS, close_count, far_count))
    counts = jnp.where(sender == receiver + 1, CAP_NEAR, counts)
    counts = jnp.where(sender == (receiver + devices_all // 2) % devices_all, CAP_FAR, counts)
    scores = jax.random.randint(keys[2], (devices_all, devices_all, CELLS_DEV), 0, 1 << 20)
    scores = scores * CELLS_DEV + jnp.arange(CELLS_DEV, dtype=jnp.int32)
    chosen = jnp.argsort(scores, axis=-1)[:, :, :CAP_NEAR].astype(jnp.int32)
    send_lists = chosen.reshape(devices_all, devices_all * CAP_NEAR)
    entries = TYPES * CELLS_DEV
    position = jnp.arange(CAP_NEAR, dtype=jnp.int32)
    usable = (position[None, None, :] < counts[:, :, None]).reshape(devices_all, devices_all * CAP_NEAR)
    codes = CELLS_DEV + jnp.arange(devices_all * CAP_NEAR, dtype=jnp.int32)
    ranks = jnp.cumsum(usable.astype(jnp.int32), axis=1) - 1
    place_scores = jax.random.randint(keys[3], (devices_all, entries - 1), 0, 1 << 14)
    place_scores = place_scores * entries + jnp.arange(entries - 1, dtype=jnp.int32)
    places = 1 + jnp.argsort(place_scores, axis=1).astype(jnp.int32)
    targets = jnp.take_along_axis(places, jnp.clip(ranks, 0, entries - 2), axis=1)
    targets = jnp.where(usable, targets, entries)
    own_cells = jax.random.randint(keys[4], (devices_all, entries), 0, CELLS_DEV)
    own_cells = own_cells.at[:, 0].set(0)
    rows = jnp.broadcast_to(receiver, targets.shape)
    filled = own_cells.at[rows, targets].set(jnp.broadcast_to(codes[None, :], targets.shape), mode='drop')
    lists = filled.reshape(devices_all, TYPES, CELLS_DEV).transpose(1, 0, 2).reshape(TYPES, devices_all * CELLS_DEV)
    return (send_lists.astype(jnp.int32), lists.astype(jnp.int32))


def draw_send_cells(key, part):
    return let_plan(key)[0]


def draw_far_list(key, part):
    return let_plan(key)[1]


def draw_near_list(key, part):
    base = jax.random.fold_in(key, 9151)
    cells_here = jnp.arange(CELLS_DEV, dtype=jnp.int32)
    jumps = jax.random.randint(base, (NEAR, N_LEAF, CELLS_DEV), -HALO, HALO + 1)
    kinds = jnp.arange(NEAR, dtype=jnp.int32)[:, None, None]
    jumps = jnp.where(kinds == NEAR // 2, 0, jumps)
    values = cells_here[None, None, :] + HALO + jumps
    values = values.at[0, :, 0].set(0)
    values = values.at[NEAR - 1, :, CELLS_DEV - 1].set(CELLS_DEV + 2 * HALO - 1)
    return values.reshape(NEAR, N_LEAF * CELLS_DEV).astype(jnp.int32)


def level_of(stream_key, extent, cuts, least, largest):
    def one(dim, shards_of):
        steps = jax.random.uniform(jax.random.fold_in(jax.random.fold_in(stream_key, 6), dim), (shards_of,), jnp.float32, least / len(cuts), largest / len(cuts))
        return jnp.repeat(jnp.exp(steps), extent[dim] // shards_of).reshape((-1,) + (1,) * (len(extent) - dim - 1))

    loudness = one(*cuts[0])
    for cut in cuts[1:]:
        loudness = loudness * one(*cut)
    return loudness


def noise(stream_key, dims, spread, bound, pieces=(), kind=jnp.bfloat16):
    values = spread * jax.random.normal(stream_key, dims, jnp.float32)
    if pieces:
        values = values * level_of(stream_key, dims, pieces, -0.22, 0.18)
    return jnp.clip(values, -bound, bound).astype(kind)


def setup_inputs(seed: int = 0) -> dict:
    key_of = jax.random.split(jax.random.key(seed), 12)
    return {
        "slip": noise(key_of[0], (ELEM, CELLS), 1.0, 6.0, ((1, 128),)),
        "to_multipole": noise(key_of[1], (COEF, ELEM), ELEM ** -0.5, 0.5),
        "up_shift": noise(key_of[2], (2, COEF, COEF), (2 * COEF) ** -0.5, 0.375, (), jnp.float32),
        "down_shift": noise(key_of[3], (2, COEF, COEF), COEF ** -0.5, 0.5, (), jnp.float32),
        "sibling_far": noise(key_of[4], (2, COEF, COEF), COEF ** -0.5, 0.5, (), jnp.float32),
        "leaf_far": noise(key_of[5], (TYPES, COEF, COEF), (4 * COEF) ** -0.5, 0.25),
        "to_stress": noise(key_of[6], (ELEM, COEF), (16 * COEF) ** -0.5, 0.125),
        "near_blocks": noise(key_of[7], (NEAR, ELEM, ELEM), (NEAR * ELEM) ** -0.5, 0.1875),
        "send_cells": draw_send_cells(jax.random.fold_in(key_of[11], 71), 0),
        "far_list": draw_far_list(jax.random.fold_in(key_of[11], 71), 0),
        "near_list": draw_near_list(jax.random.fold_in(key_of[11], 71), 0),
    }


def reference(slip, to_multipole, up_shift, down_shift, sibling_far, leaf_far, to_stress, near_blocks, send_cells, far_list, near_list):
    precise = lax.Precision.HIGHEST
    multipole = jnp.dot(to_multipole, slip, preferred_element_type=jnp.float32).astype(jnp.bfloat16)
    heights = CELLS.bit_length() - 1
    aggregates = [multipole.astype(jnp.float32)]
    for height in range(heights - 1):
        below = aggregates[-1]
        aggregates.append(jnp.dot(up_shift[0], below[:, 0::2], precision=precise)
                          + jnp.dot(up_shift[1], below[:, 1::2], precision=precise))
    expansion = jnp.zeros((COEF, 1), jnp.float32)
    for height in range(heights - 1, -1, -1):
        left_part = jnp.dot(down_shift[0], expansion, precision=precise)
        right_part = jnp.dot(down_shift[1], expansion, precision=precise)
        if height >= 1:
            level_sums = aggregates[height]
            left_part = left_part + jnp.dot(sibling_far[0], level_sums[:, 1::2], precision=precise)
            right_part = right_part + jnp.dot(sibling_far[1], level_sums[:, 0::2], precision=precise)
        expansion = jnp.stack([left_part, right_part], axis=-1).reshape(COEF, -1)
    owner = jnp.arange(CELLS, dtype=jnp.int32) // CELLS_DEV
    relative = far_list - CELLS_DEV
    sender = jnp.clip(relative // CAP_NEAR, 0, N_LEAF - 1).astype(jnp.int32)
    position = (relative % CAP_NEAR).astype(jnp.int32)
    flat_lists = send_cells.reshape(-1)
    listed = flat_lists[sender * (N_LEAF * CAP_NEAR) + owner[None, :] * CAP_NEAR + position]
    source = jnp.where(far_list < CELLS_DEV, owner[None, :] * CELLS_DEV + far_list, sender * CELLS_DEV + listed).astype(jnp.int32)
    leaf_sum = jnp.zeros((COEF, CELLS), jnp.float32)
    for kind in range(TYPES):
        leaf_sum = leaf_sum + jnp.dot(leaf_far[kind], jnp.take(multipole, source[kind], axis=1), preferred_element_type=jnp.float32)
    local_exp = (expansion + leaf_sum).astype(jnp.bfloat16)
    padded = jnp.pad(slip, ((0, 0), (HALO, HALO)))
    near_source = (owner[None, :] * CELLS_DEV + near_list).astype(jnp.int32)
    stress = jnp.dot(to_stress, local_exp, preferred_element_type=jnp.float32)
    for kind in range(NEAR):
        stress = stress + jnp.dot(near_blocks[kind], jnp.take(padded, near_source[kind], axis=1), preferred_element_type=jnp.float32)
    return stress
```

```python
import functools

import jax
import jax.numpy as jnp
from jax import lax
from jax.experimental import pallas as pl
from jax.experimental.pallas import tpu as pltpu
from jax.sharding import PartitionSpec as P

NEAR = 9
TYPES = 27
NEAR_PEERS = 4
HALO = 32
CAP_NEAR = 128
CAP_FAR = 32
EXTRA = CAP_NEAR - CAP_FAR
LANES = 128
OFFSETS = tuple(range(-NEAR_PEERS, 0)) + tuple(range(1, NEAR_PEERS + 1))

VM = pl.BlockSpec(memory_space=pltpu.VMEM)
SM = pl.BlockSpec(memory_space=pltpu.SMEM)
F32 = jnp.float32
BF16 = jnp.bfloat16
NT = (((1,), (1,)), ((), ()))
NN = (((1,), (0,)), ((), ()))


def iota(shape, dim):
    return lax.broadcasted_iota(jnp.int32, shape, dim)


def reversed_bits(value, bits):
    out = 0
    for bit in range(bits):
        out |= (value >> bit & 1) << (bits - 1 - bit)
    return out


def reversed_iota(shape, dim, bits):
    index = iota(shape, dim)
    out = jnp.zeros(shape, jnp.int32)
    for bit in range(bits):
        out = out | ((index >> bit) & 1) << (bits - 1 - bit)
    return out


def bdot(a, b, dims):
    return lax.dot_general(a, b, dims, preferred_element_type=F32)


def fdot(a, w):
    return lax.dot_general(
        a, w, NT, precision=lax.Precision.HIGHEST, preferred_element_type=F32
    )


def one_hot(column, row):
    return jnp.where(column == row, 1.0, 0.0).astype(BF16)


def padded_into(ref, block):
    ref[...] = jnp.zeros_like(ref)
    if len(block.shape) == 3:
        ref[:, : block.shape[1], : block.shape[2]] = block
    else:
        ref[: block.shape[0], : block.shape[1]] = block


def send_kernel(own, slip, to_mult, up_shift, send, *refs):
    far_out, near_outs = refs[0], refs[1 : 1 + len(OFFSETS)]
    mult_out, agg_out, tm, wu, picks = refs[1 + len(OFFSETS) :]
    cells = slip.shape[1]
    coef = to_mult.shape[0]
    devices = send.shape[0]
    bits = cells.bit_length() - 1
    padded_into(tm, to_mult[...])
    padded_into(wu, up_shift[...])
    unit = one_hot(iota((cells, cells), 0), iota((cells, cells), 1))
    slip_rows = bdot(unit, slip[...], NT).astype(BF16)
    mult = bdot(slip_rows, tm[...], NT).astype(BF16)
    mult_out[...] = mult
    flip = one_hot(reversed_iota((cells, cells), 0, bits), iota((cells, cells), 1))
    level = bdot(flip, mult, NN)
    at = 0
    rows = cells
    for _ in range(bits):
        agg_out[at : at + rows, :] = level
        at += rows
        rows //= 2
        level = fdot(level[:rows], wu[0]) + fdot(level[rows:], wu[1])
    cell_row = iota((CAP_FAR, cells), 1).astype(F32)
    lists = send[...].astype(F32).T
    group = 8
    for first in range(0, devices, group):
        hot = jnp.concatenate(
            [
                one_hot(lists[:CAP_FAR, dest : dest + 1], cell_row)
                for dest in range(first, first + group)
            ],
            axis=0,
        )
        far_out[first : first + group] = (
            bdot(hot, mult, NN).astype(BF16).reshape(group, CAP_FAR, LANES)
        )
    for slot, offset in enumerate(OFFSETS):
        dest = jnp.clip(own[0] - offset, 0, devices - 1)
        picks[slot : slot + 1, :] = send[pl.ds(dest, 1), :].astype(F32)
    chosen = jnp.concatenate([picks[...], jnp.zeros((LANES - 8, LANES), F32)], axis=0).T
    extra_row = iota((EXTRA, cells), 1).astype(F32)
    for slot, offset in enumerate(OFFSETS):
        hot = one_hot(chosen[CAP_FAR:, slot : slot + 1], extra_row)
        near_outs[slot][:EXTRA, :] = bdot(hot, mult, NN).astype(BF16)
        if offset == -1:
            near_outs[slot][EXTRA:, :] = slip_rows[cells - HALO :]
        if offset == 1:
            near_outs[slot][EXTRA:, :] = slip_rows[:HALO]
    lane = iota((LANES, LANES), 1)
    spread = one_hot(iota((LANES, LANES), 0) % 4 + coef, lane)
    own_row = (iota((CAP_FAR, LANES), 1) // 4) == iota((CAP_FAR, LANES), 0)
    placed = jnp.where(own_row, level, 0.0).astype(BF16)
    tail = bdot(placed, spread, NN).astype(BF16)
    tail_lane = iota((CAP_FAR, LANES), 1) >= coef
    for dest in range(devices):
        far_out[dest] = jnp.where(tail_lane, tail, far_out[dest])


def near_kernel(slip, low, high, lists, blocks, out, ext, cat):
    elems, cells = slip.shape
    ext[...] = jnp.zeros_like(ext)
    ext[:, :cells] = slip[...]
    ext[:, cells : cells + HALO] = low[EXTRA:, :].astype(F32).T.astype(BF16)
    ext[:, cells + HALO : cells + 2 * HALO] = high[EXTRA:, :].astype(F32).T.astype(BF16)
    span = ext.shape[1]
    at = iota((span, cells), 0)
    total = jnp.zeros((elems, cells), F32)
    for kind in range(NEAR):
        w = lists[kind : kind + 1, :]
        w = jnp.where(w < HALO, w + cells, jnp.where(w < cells + HALO, w - HALO, w))
        hot = one_hot(at, w)
        total = total + bdot(blocks[kind], bdot(ext[...], hot, NN).astype(BF16), NN)
    out[...] = total


def leaf_kernel(own, index, far, *refs):
    nears = refs[: len(OFFSETS)]
    (mult, agg, leaf_far, up_shift, down_shift, sibling, to_stress, near_part) = refs[
        len(OFFSETS) : len(OFFSETS) + 8
    ]
    out, table, wu, wd, ws, ts, total = refs[len(OFFSETS) + 8 : len(OFFSETS) + 15]
    buffers = refs[len(OFFSETS) + 15 :]
    devices = far.shape[0]
    cells = mult.shape[0]
    coef = leaf_far.shape[1]
    bits = cells.bit_length() - 1
    tree_bits = devices.bit_length() - 1
    padded_into(wu, up_shift[...])
    padded_into(wd, down_shift[...])
    padded_into(ws, sibling[...])
    padded_into(ts, to_stress[...])
    table[:cells, :] = mult[...].astype(F32)
    step = 8
    for first in range(0, devices, step):
        table[pl.ds(cells + first * CAP_FAR, step * CAP_FAR), :] = (
            far[first : first + step].reshape(step * CAP_FAR, LANES).astype(F32)
        )
    base = cells + devices * CAP_FAR
    for slot in range(len(OFFSETS)):
        table[base + slot * EXTRA : base + (slot + 1) * EXTRA, :] = nears[slot][
            :EXTRA, :
        ].astype(F32)
    spread = one_hot(iota((LANES, LANES), 0), iota((LANES, LANES), 1) % 4 + coef)
    slot_of = iota((CAP_FAR, LANES), 0)
    keep = (iota((CAP_FAR, LANES), 1) // 4 == slot_of) & (iota((CAP_FAR, LANES), 1) < coef)
    roots = bdot(far[...].reshape(devices * CAP_FAR, LANES), spread, NN)
    roots = roots.reshape(devices, CAP_FAR, LANES)
    roots = jnp.sum(jnp.where(keep[None], roots, 0.0), axis=1).astype(BF16)
    flip = one_hot(
        reversed_iota((devices, devices), 0, tree_bits), iota((devices, devices), 1)
    )
    top = [bdot(flip, roots, NN)]
    rows = devices
    for _ in range(tree_bits - 1):
        rows //= 2
        below = top[-1]
        top.append(fdot(below[:rows], wu[0]) + fdot(below[rows:], wu[1]))
    local = jnp.zeros((1, LANES), F32)
    for level in reversed(top):
        half = level.shape[0] // 2
        first = fdot(local, wd[0]) + fdot(level[half:], ws[0])
        second = fdot(local, wd[1]) + fdot(level[:half], ws[1])
        local = jnp.concatenate([first, second], axis=0)
    place = 0
    for bit in range(tree_bits):
        place = place | ((own[0] >> bit) & 1) << (tree_bits - 1 - bit)
    mine = iota((devices, LANES), 0) == place
    local = jnp.sum(jnp.where(mine, local, 0.0), axis=0, keepdims=True)
    starts = [0]
    for height in range(bits):
        starts.append(starts[-1] + (cells >> height))
    for height in reversed(range(bits)):
        first = fdot(local, wd[0])
        second = fdot(local, wd[1])
        if height >= 1:
            half = cells >> (height + 1)
            low = agg[starts[height] : starts[height] + half, :]
            high = agg[starts[height] + half : starts[height] + 2 * half, :]
            first = first + fdot(high, ws[0])
            second = second + fdot(low, ws[1])
        local = jnp.concatenate([first, second], axis=0)
    total[...] = local
    count = len(buffers)

    def step_types(step_at, carry):
        for part in range(count):
            kind = step_at * count + part
            for cell in range(cells):
                row = index[kind, cell]
                spot = reversed_bits(cell, bits)
                buffers[part][spot : spot + 1, :] = table[pl.ds(row, 1), :]
        acc = total[:, :coef]
        for part in range(count):
            kind = step_at * count + part
            acc = acc + bdot(
                buffers[part][...].astype(BF16)[:, :coef], leaf_far[kind], NT
            )
        total[:, :coef] = acc
        return carry

    lax.fori_loop(0, TYPES // count, step_types, 0)
    unflip = one_hot(reversed_iota((cells, cells), 0, bits), iota((cells, cells), 1))
    expansion = bdot(unflip, total[...].astype(BF16), NN).astype(BF16)
    out[...] = bdot(ts[...], expansion, NT) + near_part[...]


def shape(dims, dtype):
    return jax.ShapeDtypeStruct(dims, dtype)


def vmem(dims, dtype):
    return pltpu.VMEM(dims, dtype)


def body(
    slip,
    to_multipole,
    up_shift,
    down_shift,
    sibling_far,
    leaf_far,
    to_stress,
    near_blocks,
    send_cells,
    far_list,
    near_list,
):
    elems, cells = slip.shape
    coef = to_multipole.shape[0]
    devices = lax.axis_size("leaf")
    own = lax.axis_index("leaf").astype(jnp.int32)
    own_arr = own.reshape(1)
    near_rows = [EXTRA + (HALO if abs(o) == 1 else 0) for o in OFFSETS]
    outs = pl.pallas_call(
        send_kernel,
        out_shape=[shape((devices, CAP_FAR, LANES), BF16)]
        + [shape((rows, LANES), BF16) for rows in near_rows]
        + [shape((cells, LANES), BF16), shape((2 * cells, LANES), F32)],
        in_specs=[SM, VM, VM, VM, VM],
        out_specs=[VM] * (3 + len(OFFSETS)),
        scratch_shapes=[
            vmem((LANES, elems), BF16),
            vmem((2, LANES, LANES), F32),
            vmem((8, LANES), F32),
        ],
        name="send",
    )(own_arr, slip, to_multipole, up_shift, send_cells.reshape(devices, CAP_NEAR))
    far_send, near_send = outs[0], outs[1 : 1 + len(OFFSETS)]
    mult, agg = outs[1 + len(OFFSETS) :]
    far = lax.all_to_all(far_send, "leaf", split_axis=0, concat_axis=0, tiled=True)
    nears = []
    for slot, offset in enumerate(OFFSETS):
        pairs = [(i, i - offset) for i in range(devices) if 0 <= i - offset < devices]
        nears.append(lax.ppermute(near_send[slot], "leaf", pairs))
    relative = far_list - cells
    sender = relative // CAP_NEAR
    position = relative % CAP_NEAR
    apart = sender - own
    slot = jnp.where(apart < 0, apart + NEAR_PEERS, apart + NEAR_PEERS - 1)
    base = cells + devices * CAP_FAR
    far_at = cells + sender * CAP_FAR + position
    near_at = base + slot * EXTRA + position - CAP_FAR
    index = jnp.where(
        far_list < cells, far_list, jnp.where(position < CAP_FAR, far_at, near_at)
    )
    low = nears[OFFSETS.index(-1)]
    high = nears[OFFSETS.index(1)]
    near_part = pl.pallas_call(
        near_kernel,
        out_shape=shape((elems, cells), F32),
        in_specs=[VM] * 5,
        out_specs=VM,
        scratch_shapes=[vmem((elems, cells + LANES), BF16), vmem((8, LANES), BF16)],
        cost_estimate=pl.CostEstimate(
            flops=2 * 10**9, bytes_accessed=10**6, transcendentals=0
        ),
        name="near",
    )(slip, low, high, near_list, near_blocks)
    table_rows = cells + devices * CAP_FAR + len(OFFSETS) * EXTRA
    return pl.pallas_call(
        leaf_kernel,
        out_shape=shape((elems, cells), F32),
        in_specs=[SM, SM] + [VM] * (9 + len(OFFSETS)),
        out_specs=VM,
        scratch_shapes=[
            vmem((table_rows, LANES), F32),
            vmem((2, LANES, LANES), F32),
            vmem((2, LANES, LANES), F32),
            vmem((2, LANES, LANES), F32),
            vmem((elems, LANES), BF16),
            vmem((cells, LANES), F32),
        ]
        + [vmem((cells, LANES), F32)] * 3,
        name="leaf",
    )(
        own_arr,
        index,
        far,
        *nears,
        mult,
        agg,
        leaf_far,
        up_shift,
        down_shift,
        sibling_far,
        to_stress,
        near_part,
    )


def solution(mesh):
    return jax.shard_map(
        body,
        mesh=mesh,
        in_specs=(
            P(None, "leaf"),
            P(),
            P(),
            P(),
            P(),
            P(),
            P(),
            P(),
            P("leaf", None),
            P(None, "leaf"),
            P(None, "leaf"),
        ),
        out_specs=P(None, "leaf"),
        check_vma=False,
    )
```

```python
import jax
import jax.numpy as jnp
from jax import lax
from jax.experimental import pallas as pl
from jax.experimental.pallas import tpu as pltpu
from jax.sharding import PartitionSpec as P

NEAR = 9
TYPES = 27
NEAR_PEERS = 4
HALO = 32
CAP_NEAR = 128
CAP_FAR = 32
EXTRA = CAP_NEAR - CAP_FAR
LANES = 128
TRIPLE = 3 * LANES
OFFSETS = (-1, 1, -3, -4, -2, 3, 4, 2)

VM = pl.BlockSpec(memory_space=pltpu.VMEM)
SM = pl.BlockSpec(memory_space=pltpu.SMEM)
F32 = jnp.float32
BF16 = jnp.bfloat16
NT = (((1,), (1,)), ((), ()))
NN = (((1,), (0,)), ((), ()))


def iota(dims, dim):
    return lax.broadcasted_iota(jnp.int32, dims, dim)


def reversed_bits(value, bits):
    out = 0
    for bit in range(bits):
        out = out | ((value >> bit) & 1) << (bits - 1 - bit)
    return out


def bdot(a, b, dims):
    return lax.dot_general(a, b, dims, preferred_element_type=F32)


def one_hot(column, row):
    return jnp.where(column == row, 1.0, 0.0).astype(BF16)


def halves(x):
    high = x.astype(BF16)
    return high, (x - high.astype(F32)).astype(BF16)


def tripled(x):
    high, low = halves(x)
    return [high, high, low]


def lanes(parts):
    return jnp.concatenate(parts, axis=1)


def rows(parts):
    return jnp.concatenate(parts, axis=0)


def put_split(ref, at, block):
    high, low = halves(block)
    size, width = block.shape
    for part, value in enumerate((high, low, high)):
        start = at + part * LANES
        ref[:size, start : start + width] = value


def send_kernel(own, slip, to_mult, up_shift, send, far_out, up_out, down_out, plus_out,
                minus_out, mult_out, slip_out, agg_out, wu, tm, picks):
    cells = slip.shape[1]
    coef = to_mult.shape[0]
    devices = send.shape[0]
    bits = cells.bit_length() - 1
    tm[...] = jnp.zeros_like(tm)
    tm[:coef, :] = to_mult[...]
    wu[...] = jnp.zeros_like(wu)
    put_split(wu, 0, up_shift[:, 0, :])
    put_split(wu, TRIPLE, up_shift[:, 1, :])
    at_row = iota((cells, cells), 0)
    at_lane = iota((cells, cells), 1)
    slip_rows = bdot(one_hot(at_row, at_lane), slip[...], NT).astype(BF16)
    slip_out[...] = slip_rows
    mult = bdot(slip_rows, tm[...], NT).astype(BF16)
    mult_out[...] = mult
    level = bdot(one_hot(reversed_bits(at_row, bits), at_lane), mult, NN)
    start, size = 0, cells
    for _ in range(bits):
        agg_out[start : start + size, :] = level
        start += size
        size //= 2
        level = bdot(lanes(tripled(level[:size]) + tripled(level[size:])), wu[...], NT)
    cell_row = iota((CAP_FAR, cells), 1).astype(F32)
    lists = send[...].astype(F32).T
    group = 8
    for first in range(0, devices, group):
        hot = rows(
            [one_hot(lists[:CAP_FAR, d : d + 1], cell_row) for d in range(first, first + group)]
        )
        far_out[first : first + group] = (
            bdot(hot, mult, NN).astype(BF16).reshape(group, CAP_FAR, LANES)
        )
    targets = (1, 4, -2, -1, -4, 2, 3, -3)
    for slot, step in enumerate(targets):
        dest = (own[0] + step) & (devices - 1)
        picks[slot : slot + 1, :] = send[pl.ds(dest, 1), :].astype(F32)
    chosen = rows([picks[...], jnp.zeros((LANES - 8, LANES), F32)]).T
    extra_row = iota((EXTRA, cells), 1).astype(F32)
    homes = [(up_out, 0), (up_out, 1), (up_out, 2), (down_out, 0), (down_out, 1),
             (down_out, 2), (plus_out, 0), (minus_out, 0)]
    for slot, (ref, place) in enumerate(homes):
        hot = one_hot(chosen[CAP_FAR:, slot : slot + 1], extra_row)
        ref[place * EXTRA : (place + 1) * EXTRA, :] = bdot(hot, mult, NN).astype(BF16)
    up_out[3 * EXTRA :, :] = slip_rows[cells - HALO :]
    down_out[3 * EXTRA :, :] = slip_rows[:HALO]
    spread = one_hot(iota((LANES, LANES), 0) % 4 + coef, iota((LANES, LANES), 1))
    own_row = (iota((CAP_FAR, LANES), 1) // 4) == iota((CAP_FAR, LANES), 0)
    placed = jnp.where(own_row, level, 0.0).astype(BF16)
    tail = bdot(placed, spread, NN).astype(BF16)
    tail_lane = iota((CAP_FAR, LANES), 1) >= coef
    for dest in range(devices):
        far_out[dest] = jnp.where(tail_lane, tail, far_out[dest])


def tree_kernel(own, far_list, agg, down_shift, sibling, index_out, local_out, w0, w1):
    cells = far_list.shape[1]
    kinds = far_list.shape[0]
    bits = cells.bit_length() - 1
    devices = LANES
    value = far_list[...]
    relative = value - cells
    sender = relative >> 7
    position = relative & (CAP_NEAR - 1)
    apart = sender - own[0]
    slot = jnp.zeros_like(value)
    for place, offset in enumerate(OFFSETS):
        slot = jnp.where(apart == offset, place, slot)
    far_at = cells + sender * CAP_FAR + position
    near_at = cells + devices * CAP_FAR + slot * EXTRA + position - CAP_FAR
    mapped = jnp.where(value < cells, value, jnp.where(position < CAP_FAR, far_at, near_at))
    for part in range(cells // LANES):
        index_out[pl.ds(part, kinds, stride=cells // LANES), :] = mapped[
            :, part * LANES : (part + 1) * LANES
        ]
    for ref, which in ((w0, 0), (w1, 1)):
        ref[...] = jnp.zeros_like(ref)
        put_split(ref, 0, down_shift[:, which, :])
        put_split(ref, TRIPLE, sibling[:, which, :])
    starts = [0]
    for height in range(bits):
        starts.append(starts[-1] + (cells >> height))
    local = None
    for height in reversed(range(bits)):
        parts = []
        for which, weights in ((0, w0), (1, w1)):
            total = None
            if local is not None:
                total = bdot(lanes(tripled(local)), weights[:, :TRIPLE], NT)
            if height >= 1:
                half = cells >> (height + 1)
                at = starts[height] + (1 - which) * half
                other = bdot(
                    lanes(tripled(agg[at : at + half, :])), weights[:, TRIPLE:], NT
                )
                total = other if total is None else total + other
            parts.append(total)
        local = rows(parts)
    local_out[...] = local


def near_kernel(own, slip_rows, low, high, lists, blocks, out, ext, columns):
    cells, elems = slip_rows.shape
    last = LANES - 1
    ext[...] = jnp.zeros_like(ext)
    ext[:HALO, :] = jnp.where(own[0] == 0, 0.0, low[3 * EXTRA :, :].astype(F32)).astype(BF16)
    ext[HALO : HALO + cells, :] = slip_rows[...]
    ext[HALO + cells : 2 * HALO + cells, :] = jnp.where(
        own[0] == last, 0.0, high[3 * EXTRA :, :].astype(F32)
    ).astype(BF16)
    columns[...] = jnp.zeros_like(columns)
    columns[: lists.shape[0], :] = lists[...].astype(F32)
    turned = columns[...].T
    at_lane = iota((cells, ext.shape[0]), 1).astype(F32)
    total = jnp.zeros((cells, elems), F32)
    for kind in range(NEAR):
        hot = one_hot(turned[:, kind : kind + 1], at_lane)
        gathered = bdot(hot, ext[...], NN).astype(BF16)
        total = total + bdot(gathered, blocks[kind], NT)
    out[...] = total.T


def leaf_kernel(own, index, far, low, high, plus, minus, mult, wu, w0, w1, leaf_far,
                to_stress, local_own, near_part, out, table, levels, ts, *buffers):
    devices = far.shape[0]
    cells = mult.shape[0]
    coef = leaf_far.shape[1]
    bits = cells.bit_length() - 1
    tree_bits = devices.bit_length() - 1
    ts[...] = jnp.zeros_like(ts)
    ts[:, :coef] = to_stress[...]
    table[:cells, :] = mult[...].astype(F32)
    step = 8
    for first in range(0, devices, step):
        table[cells + first * CAP_FAR : cells + (first + step) * CAP_FAR, :] = (
            far[first : first + step].reshape(step * CAP_FAR, LANES).astype(F32)
        )
    at = cells + devices * CAP_FAR
    for block in (low[:EXTRA, :], high[:EXTRA, :], plus[...], minus[...]):
        table[at : at + block.shape[0], :] = block.astype(F32)
        at += block.shape[0]

    spread = one_hot(iota((LANES, LANES), 0), iota((LANES, LANES), 1) % 4 + coef)
    keep = (iota((CAP_FAR, LANES), 1) // 4 == iota((CAP_FAR, LANES), 0)) & (
        iota((CAP_FAR, LANES), 1) < coef
    )
    roots = bdot(far[...].reshape(devices * CAP_FAR, LANES), spread, NN)
    roots = roots.reshape(devices, CAP_FAR, LANES)
    roots = jnp.sum(jnp.where(keep[None], roots, 0.0), axis=1).astype(BF16)
    square = (devices, devices)
    flip = one_hot(reversed_bits(iota(square, 0), tree_bits), iota(square, 1))
    level = bdot(flip, roots, NN)
    start, size = 0, devices
    starts = []
    for depth in range(tree_bits):
        levels[start : start + size, :] = level
        starts.append(start)
        start += size
        size //= 2
        if depth + 1 < tree_bits:
            level = bdot(lanes(tripled(level[:size]) + tripled(level[size:])), wu[...], NT)
    local = jnp.zeros((1, LANES), F32)
    for depth in reversed(range(tree_bits)):
        node = own[0] >> depth
        place = starts[depth] + reversed_bits(node ^ 1, tree_bits - depth)
        other = levels[pl.ds(place, 1), :]
        stacked = lanes(tripled(local) + tripled(other))
        first = bdot(stacked, w0[...], NT)
        second = bdot(stacked, w1[...], NT)
        local = jnp.where((node & 1) == 0, first, second)
    for _ in range(bits):
        stacked = lanes(tripled(local))
        local = rows([bdot(stacked, w0[:, :TRIPLE], NT), bdot(stacked, w1[:, :TRIPLE], NT)])
    total = local_own[...] + local
    count = len(buffers)
    total = total[:, :coef]
    for kind in range(TYPES):
        buffer = buffers[kind % count]
        for cell in range(cells):
            row = index[kind * cells + cell]
            spot = reversed_bits(cell, bits)
            buffer[spot : spot + 1, :] = table[pl.ds(row, 1), :]
        total = total + bdot(buffer[...].astype(BF16)[:, :coef], leaf_far[kind], NT)
    unflip = one_hot(reversed_bits(iota((cells, cells), 0), bits), iota((cells, cells), 1))
    expansion = bdot(unflip, total.astype(BF16), NN).astype(BF16)
    out[...] = bdot(ts[:, :coef], expansion, NT) + near_part[...]


def shape(dims, dtype):
    return jax.ShapeDtypeStruct(dims, dtype)


def scratch(dims, dtype):
    return pltpu.VMEM(dims, dtype)


def cost(flops):
    return pl.CostEstimate(flops=flops, bytes_accessed=10**6, transcendentals=0)


def shifted(block, by):
    count = lax.axis_size("leaf")
    return lax.ppermute(block, "leaf", [(i, (i + by) % count) for i in range(count)])


def body(
    slip,
    to_multipole,
    up_shift,
    down_shift,
    sibling_far,
    leaf_far,
    to_stress,
    near_blocks,
    send_cells,
    far_list,
    near_list,
):
    elems, cells = slip.shape
    devices = lax.axis_size("leaf")
    own = lax.axis_index("leaf").astype(jnp.int32).reshape(1)
    up_t, down_t, sibling_t = (
        jnp.transpose(w, (1, 0, 2)) for w in (up_shift, down_shift, sibling_far)
    )
    bundle = 3 * EXTRA + HALO
    far_send, up_send, down_send, plus_own, minus_own, mult, slip_rows, agg, wu = pl.pallas_call(
        send_kernel,
        out_shape=[
            shape((devices, CAP_FAR, LANES), BF16),
            shape((bundle, LANES), BF16),
            shape((bundle, LANES), BF16),
            shape((EXTRA, LANES), BF16),
            shape((EXTRA, LANES), BF16),
            shape((cells, LANES), BF16),
            shape((cells, elems), BF16),
            shape((2 * cells, LANES), F32),
            shape((LANES, 2 * TRIPLE), BF16),
        ],
        in_specs=[SM, VM, VM, VM, VM],
        out_specs=[VM] * 9,
        scratch_shapes=[scratch((LANES, elems), BF16), scratch((8, LANES), F32)],
        name="send",
    )(own, slip, to_multipole, up_t, send_cells.reshape(devices, CAP_NEAR))
    far = lax.all_to_all(far_send, "leaf", split_axis=0, concat_axis=0, tiled=True)
    low = shifted(up_send, 1)
    high = shifted(down_send, -1)
    plus = shifted(
        rows([plus_own, low[EXTRA : 2 * EXTRA], high[2 * EXTRA : 3 * EXTRA]]), 3
    )
    minus = shifted(
        rows([minus_own, high[EXTRA : 2 * EXTRA], low[2 * EXTRA : 3 * EXTRA]]), -3
    )
    index_rows = (TYPES * cells // LANES + 7) // 8 * 8
    index, local_own, w0, w1 = pl.pallas_call(
        tree_kernel,
        out_shape=[
            shape((index_rows, LANES), jnp.int32),
            shape((cells, LANES), F32),
            shape((LANES, 2 * TRIPLE), BF16),
            shape((LANES, 2 * TRIPLE), BF16),
        ],
        in_specs=[SM, VM, VM, VM, VM],
        out_specs=[VM] * 4,
        cost_estimate=cost(10**9),
        name="tree",
    )(own, far_list, agg, down_t, sibling_t)
    near_part = pl.pallas_call(
        near_kernel,
        out_shape=shape((elems, cells), F32),
        in_specs=[SM] + [VM] * 5,
        out_specs=VM,
        scratch_shapes=[scratch((TRIPLE, elems), BF16), scratch((LANES, cells), F32)],
        cost_estimate=cost(10**9),
        name="near",
    )(own, slip_rows, low, high, near_list, near_blocks)
    table_rows = cells + devices * CAP_FAR + len(OFFSETS) * EXTRA
    return pl.pallas_call(
        leaf_kernel,
        out_shape=shape((elems, cells), F32),
        in_specs=[SM, SM] + [VM] * 13,
        out_specs=VM,
        scratch_shapes=[
            scratch((table_rows, LANES), F32),
            scratch((2 * devices, LANES), F32),
            scratch((elems, LANES), BF16),
        ]
        + [scratch((cells, LANES), F32)] * 6,
        name="leaf",
    )(
        own,
        index.reshape(-1),
        far,
        low,
        high,
        plus,
        minus,
        mult,
        wu,
        w0,
        w1,
        leaf_far,
        to_stress,
        local_own,
        near_part,
    )


def solution(mesh):
    return jax.shard_map(
        body,
        mesh=mesh,
        in_specs=(
            P(None, "leaf"),
            P(),
            P(),
            P(),
            P(),
            P(),
            P(),
            P(),
            P("leaf", None),
            P(None, "leaf"),
            P(None, "leaf"),
        ),
        out_specs=P(None, "leaf"),
        check_vma=False,
    )
```

```python
import jax
import jax.numpy as jnp
from jax import lax
from jax.experimental import pallas as pl
from jax.experimental.pallas import tpu as pltpu
from jax.sharding import PartitionSpec as P


NEAR = 9
TYPES = 27
HALO = 32
CAP_NEAR = 128
CAP_FAR = 32
EXTRA = CAP_NEAR - CAP_FAR
LANES = 128
TRIPLE = 3 * LANES
GROUP = 8
MIX = 100
OFFSETS = (-1, 1, -3, -4, -2, 3, 4, 2)

VM = pl.BlockSpec(memory_space=pltpu.VMEM)
SM = pl.BlockSpec(memory_space=pltpu.SMEM)
F32 = jnp.float32
BF16 = jnp.bfloat16
NT = (((1,), (1,)), ((), ()))
NN = (((1,), (0,)), ((), ()))


def iota(dims, dim):
    return lax.broadcasted_iota(jnp.int32, dims, dim)


def reversed_bits(value, bits):
    out = 0
    for bit in range(bits):
        out = out | ((value >> bit) & 1) << (bits - 1 - bit)
    return out


def bdot(a, b, dims):
    return lax.dot_general(a, b, dims, preferred_element_type=F32)


def one_hot(column, row):
    return jnp.where(column == row, 1.0, 0.0).astype(BF16)


def halves(x):
    high = x.astype(BF16)
    return high, (x - high.astype(F32)).astype(BF16)


def tripled(x):
    high, low = halves(x)
    return [high, high, low]


def lanes(parts):
    return jnp.concatenate(parts, axis=1)


def rows(parts):
    return jnp.concatenate(parts, axis=0)


def put_split(ref, at, block, square):
    square[: block.shape[0], : block.shape[1]] = block
    high, low = halves(square[...])
    for part, value in enumerate((high, low, high)):
        start = at + part * LANES
        ref[:, start : start + LANES] = value


def bit_order(size, bits):
    inner = reversed_bits(iota((8, size), 0), 3) << (bits - 3)
    gap = iota((8, size), 1) - inner
    blocks = [
        jnp.where(gap == reversed_bits(block, bits - 3), 1.0, 0.0) for block in range(size // 8)
    ]
    return rows(blocks).astype(BF16)


def matches(picked, spare, cells):
    at = iota((LANES, cells), 0)
    return jnp.where(
        at == spare, -iota((LANES, cells), 1).astype(F32), jnp.where(picked(at), 1.0, 0.0)
    ).astype(BF16)


def send_kernel(own, slip, to_mult, up_shift, send, far_out, up_out, down_out, plus_out,
                minus_out, mult_out, slip_out, agg_out, wu, tm, lists, square):
    cells = slip.shape[1]
    coef = to_mult.shape[0]
    devices = send.shape[0]
    bits = cells.bit_length() - 1
    tm[...] = jnp.zeros_like(tm)
    tm[:coef, :] = to_mult[...]
    square[...] = jnp.zeros_like(square)
    put_split(wu, 0, up_shift[:, 0, :], square)
    put_split(wu, TRIPLE, up_shift[:, 1, :], square)
    unit = one_hot(iota((cells, cells), 0), iota((cells, cells), 1))
    slip_rows = bdot(unit, slip[...], NT).astype(BF16)
    slip_out[...] = slip_rows
    mult = bdot(slip_rows, tm[...], NT).astype(BF16)
    mult_out[...] = mult
    lists[...] = send[...].astype(F32)
    level = bdot(bit_order(cells, bits), mult, NN)
    start, size = 0, cells
    for _ in range(bits):
        agg_out[start : start + size, :] = level
        start += size
        size //= 2
        level = bdot(lanes(tripled(level[:size]) + tripled(level[size:])), wu[...], NT)
    spread = one_hot(iota((LANES, LANES), 0) % 4 + coef, iota((LANES, LANES), 1))
    own_row = (iota((CAP_FAR, LANES), 1) // 4) == iota((CAP_FAR, LANES), 0)
    placed = jnp.where(own_row, level, 0.0).astype(BF16)
    tail = rows([bdot(placed, spread, NN)] * GROUP)
    lane = iota((CAP_FAR, LANES), 1)
    own_slot = lane == iota((CAP_FAR, LANES), 0)
    rest = jnp.where(lane == CAP_FAR, 1.0, 0.0)
    far_match = matches(lambda at: at < CAP_FAR, CAP_FAR, cells)
    cell_row = iota((CAP_FAR, cells), 1).astype(F32)
    turned = lists[...].T
    for first in range(0, devices, GROUP):
        group = range(first, first + GROUP)
        if first // GROUP % MIX == 0:
            hot = rows([one_hot(turned[:CAP_FAR, d : d + 1], cell_row) for d in group])
        else:
            spots = rows([jnp.where(own_slot, lists[d : d + 1, :], rest) for d in group])
            hot = one_hot(bdot(spots.astype(BF16), far_match, NN), 0.0)
        far_out[first : first + GROUP] = (
            (bdot(hot, mult, NN) + tail).astype(BF16).reshape(GROUP, CAP_FAR, LANES)
        )
    lane = iota((EXTRA, LANES), 1)
    own_slot = lane == iota((EXTRA, LANES), 0) + CAP_FAR
    rest = jnp.where(lane == 0, 1.0, 0.0)
    near_match = matches(lambda at: at >= CAP_FAR, 0, cells)
    homes = [(up_out, 0, 1), (up_out, 1, 4), (up_out, 2, -2), (down_out, 0, -1),
             (down_out, 1, -4), (down_out, 2, 2), (plus_out, 0, 3), (minus_out, 0, -3)]
    for ref, place, step in homes:
        dest = (own[0] + step) & (devices - 1)
        spots = jnp.where(own_slot, lists[pl.ds(dest, 1), :], rest).astype(BF16)
        hot = one_hot(bdot(spots, near_match, NN), 0.0)
        ref[place * EXTRA : (place + 1) * EXTRA, :] = bdot(hot, mult, NN).astype(BF16)
    up_out[3 * EXTRA :, :] = slip_rows[cells - HALO :]
    down_out[3 * EXTRA :, :] = slip_rows[:HALO]


def tree_kernel(own, far_list, agg, down_shift, sibling, index_out, local_out, w0, w1, square):
    cells = far_list.shape[1]
    kinds = far_list.shape[0]
    bits = cells.bit_length() - 1
    devices = LANES
    value = far_list[...]
    relative = value - cells
    sender = relative >> 7
    position = relative & (CAP_NEAR - 1)
    apart = sender - own[0]
    slot = jnp.zeros_like(value)
    for place, offset in enumerate(OFFSETS):
        slot = jnp.where(apart == offset, place, slot)
    far_at = cells + sender * CAP_FAR + position
    near_at = cells + devices * CAP_FAR + slot * EXTRA + position - CAP_FAR
    mapped = jnp.where(value < cells, value, jnp.where(position < CAP_FAR, far_at, near_at))
    for part in range(cells // LANES):
        index_out[pl.ds(part, kinds, stride=cells // LANES), :] = mapped[
            :, part * LANES : (part + 1) * LANES
        ]
    square[...] = jnp.zeros_like(square)
    for ref, which in ((w0, 0), (w1, 1)):
        put_split(ref, 0, down_shift[:, which, :], square)
        put_split(ref, TRIPLE, sibling[:, which, :], square)
    starts = [0]
    for height in range(bits):
        starts.append(starts[-1] + (cells >> height))
    local = None
    for height in reversed(range(bits)):
        parts = []
        for which, weights in ((0, w0), (1, w1)):
            total = None
            if local is not None:
                total = bdot(lanes(tripled(local)), weights[:, :TRIPLE], NT)
            if height >= 1:
                half = cells >> (height + 1)
                at = starts[height] + (1 - which) * half
                other = bdot(
                    lanes(tripled(agg[at : at + half, :])), weights[:, TRIPLE:], NT
                )
                total = other if total is None else total + other
            parts.append(total)
        local = rows(parts)
    local_out[...] = local


def near_kernel(own, slip_rows, low, high, lists, blocks, out, ext, columns):
    cells, elems = slip_rows.shape
    last = LANES - 1
    ext[...] = jnp.zeros_like(ext)
    ext[:HALO, :] = jnp.where(own[0] == 0, 0.0, low[3 * EXTRA :, :].astype(F32)).astype(BF16)
    ext[HALO : HALO + cells, :] = slip_rows[...]
    ext[HALO + cells : 2 * HALO + cells, :] = jnp.where(
        own[0] == last, 0.0, high[3 * EXTRA :, :].astype(F32)
    ).astype(BF16)
    columns[...] = jnp.zeros_like(columns)
    columns[: lists.shape[0], :] = lists[...].astype(F32)
    turned = columns[...].T
    at_lane = iota((cells, ext.shape[0]), 1).astype(F32)
    total = jnp.zeros((cells, elems), F32)
    for kind in range(NEAR):
        hot = one_hot(turned[:, kind : kind + 1], at_lane)
        gathered = bdot(hot, ext[...], NN).astype(BF16)
        total = total + bdot(gathered, blocks[kind], NT)
    out[...] = total.T


def top_levels(own, far, wu, w0, w1, levels, coef, bits, tree_bits, result):
    devices = far.shape[0]
    spread = one_hot(iota((LANES, LANES), 0), iota((LANES, LANES), 1) % 4 + coef)
    keep = (iota((CAP_FAR, LANES), 1) // 4 == iota((CAP_FAR, LANES), 0)) & (
        iota((CAP_FAR, LANES), 1) < coef
    )
    roots = bdot(far[...].reshape(devices * CAP_FAR, LANES), spread, NN)
    roots = roots.reshape(devices, CAP_FAR, LANES)
    roots = jnp.sum(jnp.where(keep[None], roots, 0.0), axis=1).astype(BF16)
    level = bdot(bit_order(devices, tree_bits), roots, NN)
    yield
    start, size = 0, devices
    starts = []
    for depth in range(tree_bits):
        levels[start : start + size, :] = level
        starts.append(start)
        start += size
        size //= 2
        if depth + 1 < tree_bits:
            level = bdot(lanes(tripled(level[:size]) + tripled(level[size:])), wu[...], NT)
            yield
    local = jnp.zeros((1, LANES), F32)
    for depth in reversed(range(tree_bits)):
        node = own[0] >> depth
        place = starts[depth] + reversed_bits(node ^ 1, tree_bits - depth)
        other = levels[pl.ds(place, 1), :]
        stacked = lanes(tripled(local) + tripled(other))
        first = bdot(stacked, w0[...], NT)
        second = bdot(stacked, w1[...], NT)
        local = jnp.where((node & 1) == 0, first, second)
        yield
    for step in range(bits):
        stacked = lanes(tripled(local))
        local = rows([bdot(stacked, w0[:, :TRIPLE], NT), bdot(stacked, w1[:, :TRIPLE], NT)])
        if step + 1 == bits:
            result.append(local)
        yield


def leaf_kernel(own, index_rows, far, low, high, plus, minus, mult, wu, w0, w1, leaf_far,
                to_stress, local_own, near_part, out, index, arrived, table, levels, ts,
                *buffers):
    devices = far.shape[0]
    cells = mult.shape[0]
    coef = leaf_far.shape[1]
    bits = cells.bit_length() - 1
    tree_bits = devices.bit_length() - 1
    load = pltpu.make_async_copy(index_rows, index, arrived)
    load.start()
    ts[...] = jnp.zeros_like(ts)
    ts[:, :coef] = to_stress[...]
    table[:cells, :] = mult[...].astype(F32)
    step = 8
    for first in range(0, devices, step):
        table[cells + first * CAP_FAR : cells + (first + step) * CAP_FAR, :] = (
            far[first : first + step].reshape(step * CAP_FAR, LANES).astype(F32)
        )
    at = cells + devices * CAP_FAR
    for block in (low[:EXTRA, :], high[:EXTRA, :], plus[...], minus[...]):
        table[at : at + block.shape[0], :] = block.astype(F32)
        at += block.shape[0]

    load.wait()
    result = []
    tree = top_levels(own, far, wu, w0, w1, levels, coef, bits, tree_bits, result)
    count = len(buffers)
    total = local_own[:, :coef]
    for kind in range(TYPES):
        buffer = buffers[kind % count]
        for cell in range(cells):
            spot = kind * cells + cell
            row = index[spot // LANES, spot % LANES]
            spot = reversed_bits(cell, bits)
            buffer[spot : spot + 1, :] = table[pl.ds(row, 1), :]
        total = total + bdot(buffer[...].astype(BF16)[:, :coef], leaf_far[kind], NT)
        next(tree, None)
    total = total + result[0][:, :coef]
    expansion = bdot(bit_order(cells, bits), total.astype(BF16), NN).astype(BF16)
    out[...] = bdot(ts[:, :coef], expansion, NT) + near_part[...]


def shape(dims, dtype):
    return jax.ShapeDtypeStruct(dims, dtype)


def kept(dims, dtype):
    return pltpu.VMEM(dims, dtype)


def held(x):
    return pltpu.with_memory_space_constraint(x, pltpu.VMEM)


def limits(mib):
    return pltpu.CompilerParams(vmem_limit_bytes=mib << 20)


def scratch(dims, dtype):
    return pltpu.VMEM(dims, dtype)


def cost(flops):
    return pl.CostEstimate(flops=flops, bytes_accessed=10**6, transcendentals=0)


def shifted(block, by):
    count = lax.axis_size("leaf")
    return lax.ppermute(block, "leaf", [(i, (i + by) % count) for i in range(count)])


def body(
    slip,
    to_multipole,
    up_shift,
    down_shift,
    sibling_far,
    leaf_far,
    to_stress,
    near_blocks,
    send_cells,
    far_list,
    near_list,
):
    elems, cells = slip.shape
    devices = lax.axis_size("leaf")
    own = lax.axis_index("leaf").astype(jnp.int32).reshape(1)
    up_t, down_t, sibling_t = (
        jnp.transpose(w, (1, 0, 2)) for w in (up_shift, down_shift, sibling_far)
    )
    bundle = 3 * EXTRA + HALO
    far_send, up_send, down_send, plus_own, minus_own, mult, slip_rows, agg, wu = pl.pallas_call(
        send_kernel,
        out_shape=[
            kept((devices, CAP_FAR, LANES), BF16),
            kept((bundle, LANES), BF16),
            kept((bundle, LANES), BF16),
            kept((EXTRA, LANES), BF16),
            kept((EXTRA, LANES), BF16),
            kept((cells, LANES), BF16),
            kept((cells, elems), BF16),
            kept((2 * cells, LANES), F32),
            kept((LANES, 2 * TRIPLE), BF16),
        ],
        in_specs=[SM, VM, VM, VM, VM],
        out_specs=[VM] * 9,
        scratch_shapes=[
            scratch((LANES, elems), BF16),
            scratch((devices, CAP_NEAR), F32),
            scratch((LANES, LANES), F32),
        ],
        name="send",
    )(own, slip, to_multipole, up_t, send_cells.reshape(devices, CAP_NEAR))
    low = shifted(up_send, 1)
    high = shifted(down_send, -1)
    far = lax.all_to_all(far_send, "leaf", split_axis=0, concat_axis=0, tiled=True)
    plus = shifted(
        rows([plus_own, low[EXTRA : 2 * EXTRA], high[2 * EXTRA : 3 * EXTRA]]), 3
    )
    minus = shifted(
        rows([minus_own, high[EXTRA : 2 * EXTRA], low[2 * EXTRA : 3 * EXTRA]]), -3
    )
    index_rows = (TYPES * cells // LANES + 7) // 8 * 8
    index, local_own, w0, w1 = pl.pallas_call(
        tree_kernel,
        out_shape=[
            kept((index_rows, LANES), jnp.int32),
            kept((cells, LANES), F32),
            kept((LANES, 2 * TRIPLE), BF16),
            kept((LANES, 2 * TRIPLE), BF16),
        ],
        in_specs=[SM, VM, VM, VM, VM],
        out_specs=[VM] * 4,
        scratch_shapes=[scratch((LANES, LANES), F32)],
        cost_estimate=cost(10**9),
        compiler_params=limits(16),
        name="tree",
    )(own, far_list, held(agg), down_t, sibling_t)
    near_part = pl.pallas_call(
        near_kernel,
        out_shape=kept((elems, cells), F32),
        in_specs=[SM] + [VM] * 5,
        out_specs=VM,
        scratch_shapes=[scratch((TRIPLE, elems), BF16), scratch((LANES, cells), F32)],
        cost_estimate=cost(10**9),
        compiler_params=limits(16),
        name="near",
    )(own, held(slip_rows), held(low), held(high), near_list, held(near_blocks))
    table_rows = cells + devices * CAP_FAR + len(OFFSETS) * EXTRA
    return pl.pallas_call(
        leaf_kernel,
        out_shape=shape((elems, cells), F32),
        in_specs=[SM] + [VM] * 14,
        out_specs=VM,
        scratch_shapes=[
            pltpu.SMEM((index_rows, LANES), jnp.int32),
            pltpu.SemaphoreType.DMA,
            scratch((table_rows, LANES), F32),
            scratch((2 * devices, LANES), F32),
            scratch((elems, LANES), BF16),
        ]
        + [scratch((cells, LANES), F32)] * 6,
        compiler_params=limits(24),
        name="leaf",
    )(
        own,
        held(index),
        held(far),
        held(low),
        held(high),
        held(plus),
        held(minus),
        held(mult),
        held(wu),
        held(w0),
        held(w1),
        held(leaf_far),
        held(to_stress),
        held(local_own),
        held(near_part),
    )


def solution(mesh):
    return jax.shard_map(
        body,
        mesh=mesh,
        in_specs=(
            P(None, "leaf"),
            P(),
            P(),
            P(),
            P(),
            P(),
            P(),
            P(),
            P("leaf", None),
            P(None, "leaf"),
            P(None, "leaf"),
        ),
        out_specs=P(None, "leaf"),
        check_vma=False,
    )
```

```python
import jax
import jax.numpy as jnp
from jax import lax
from jax.experimental import pallas as pl
from jax.experimental.pallas import tpu as pltpu
from jax.sharding import PartitionSpec as P


NEAR = 9
TYPES = 27
HALO = 32
CAP_NEAR = 128
CAP_FAR = 32
EXTRA = CAP_NEAR - CAP_FAR
LANES = 128
PAIR = 2 * LANES
GROUP = 8
MIX = 100
OFFSETS = (-1, 1, -3, -4, -2, 3, 4, 2)

VM = pl.BlockSpec(memory_space=pltpu.VMEM)
SM = pl.BlockSpec(memory_space=pltpu.SMEM)
F32 = jnp.float32
BF16 = jnp.bfloat16
NT = (((1,), (1,)), ((), ()))
NN = (((1,), (0,)), ((), ()))


def iota(dims, dim):
    return lax.broadcasted_iota(jnp.int32, dims, dim)


def reversed_bits(value, bits):
    out = 0
    for bit in range(bits):
        out = out | ((value >> bit) & 1) << (bits - 1 - bit)
    return out


def bdot(a, b, dims):
    return lax.dot_general(a, b, dims, preferred_element_type=F32)


def one_hot(column, row):
    return jnp.where(column == row, 1.0, 0.0).astype(BF16)


def halves(x):
    high = x.astype(BF16)
    return high, (x - high.astype(F32)).astype(BF16)


def tripled(x):
    high, low = halves(x)
    return [high, high, low]


def lanes(parts):
    return jnp.concatenate(parts, axis=1)


def rows(parts):
    return jnp.concatenate(parts, axis=0)


def put_split(ref, at, block, square):
    square[: block.shape[0], : block.shape[1]] = block
    high, low = halves(square[...])
    ref[:, at : at + LANES] = high
    ref[:, at + LANES : at + PAIR] = low


def weights(ref, *starts):
    parts = []
    for at in starts:
        high = ref[:, at : at + LANES]
        parts += [high, ref[:, at + LANES : at + PAIR], high]
    return lanes(parts)


def bit_order(size, bits):
    inner = reversed_bits(iota((8, size), 0), 3) << (bits - 3)
    gap = iota((8, size), 1) - inner
    blocks = [
        jnp.where(gap == reversed_bits(block, bits - 3), 1.0, 0.0) for block in range(size // 8)
    ]
    return rows(blocks).astype(BF16)


def matches(picked, spare, cells):
    at = iota((LANES, cells), 0)
    return jnp.where(
        at == spare, -iota((LANES, cells), 1).astype(F32), jnp.where(picked(at), 1.0, 0.0)
    ).astype(BF16)


def send_kernel(own, slip, to_mult, up_shift, send, far_hbm, up_out, down_out, plus_out,
                minus_out, mult_out, slip_out, agg_out, wu, far_out, sent, tm,
                lists, square):
    cells = slip.shape[1]
    coef = to_mult.shape[0]
    devices = send.shape[0]
    bits = cells.bit_length() - 1
    tm[...] = jnp.zeros_like(tm)
    tm[:coef, :] = to_mult[...]
    square[...] = jnp.zeros_like(square)
    put_split(wu, 0, up_shift[:, 0, :], square)
    put_split(wu, PAIR, up_shift[:, 1, :], square)
    unit = one_hot(iota((cells, cells), 0), iota((cells, cells), 1))
    slip_rows = bdot(unit, slip[...], NT).astype(BF16)
    slip_out[...] = slip_rows
    mult = bdot(slip_rows, tm[...], NT).astype(BF16)
    mult_out[...] = mult
    lists[...] = send[...].astype(F32)
    level = bdot(bit_order(cells, bits), mult, NN)
    start, size = 0, cells
    for _ in range(bits):
        agg_out[start : start + size, :] = level
        start += size
        size //= 2
        level = bdot(
            lanes(tripled(level[:size]) + tripled(level[size:])), weights(wu, 0, PAIR), NT
        )
    spread = one_hot(iota((LANES, LANES), 0) % 4 + coef, iota((LANES, LANES), 1))
    own_row = (iota((CAP_FAR, LANES), 1) // 4) == iota((CAP_FAR, LANES), 0)
    placed = jnp.where(own_row, level, 0.0).astype(BF16)
    tail = rows([bdot(placed, spread, NN)] * GROUP)
    lane = iota((CAP_FAR, LANES), 1)
    own_slot = lane == iota((CAP_FAR, LANES), 0)
    rest = jnp.where(lane == CAP_FAR, 1.0, 0.0)
    far_match = matches(lambda at: at < CAP_FAR, CAP_FAR, cells)
    cell_row = iota((CAP_FAR, cells), 1).astype(F32)
    turned = lists[...].T
    copies = []
    for first in range(0, devices, GROUP):
        group = range(first, first + GROUP)
        if first // GROUP % MIX == 0:
            hot = rows([one_hot(turned[:CAP_FAR, d : d + 1], cell_row) for d in group])
        else:
            spots = rows([jnp.where(own_slot, lists[d : d + 1, :], rest) for d in group])
            hot = one_hot(bdot(spots.astype(BF16), far_match, NN), 0.0)
        far_out[first : first + GROUP] = (
            (bdot(hot, mult, NN) + tail).astype(BF16).reshape(GROUP, CAP_FAR, LANES)
        )
        copies.append(
            pltpu.make_async_copy(
                far_out.at[pl.ds(first, GROUP)],
                far_hbm.at[pl.ds(first, GROUP)],
                sent.at[first // GROUP],
            )
        )
        copies[-1].start()
    lane = iota((EXTRA, LANES), 1)
    own_slot = lane == iota((EXTRA, LANES), 0) + CAP_FAR
    rest = jnp.where(lane == 0, 1.0, 0.0)
    near_match = matches(lambda at: at >= CAP_FAR, 0, cells)
    homes = [(up_out, 0, 1), (up_out, 1, 4), (up_out, 2, -2), (down_out, 0, -1),
             (down_out, 1, -4), (down_out, 2, 2), (plus_out, 0, 3), (minus_out, 0, -3)]
    for ref, place, step in homes:
        dest = (own[0] + step) & (devices - 1)
        spots = jnp.where(own_slot, lists[pl.ds(dest, 1), :], rest).astype(BF16)
        hot = one_hot(bdot(spots, near_match, NN), 0.0)
        ref[place * EXTRA : (place + 1) * EXTRA, :] = bdot(hot, mult, NN).astype(BF16)
    up_out[3 * EXTRA :, :] = slip_rows[cells - HALO :]
    down_out[3 * EXTRA :, :] = slip_rows[:HALO]
    for copy in copies:
        copy.wait()


def tree_kernel(own, far_list, agg, down_shift, sibling, index_out, local_out, wd, path, ws,
                square):
    cells = far_list.shape[1]
    kinds = far_list.shape[0]
    bits = cells.bit_length() - 1
    devices = LANES
    value = far_list[...]
    relative = value - cells
    sender = relative >> 7
    position = relative & (CAP_NEAR - 1)
    apart = sender - own[0]
    slot = jnp.zeros_like(value)
    for place, offset in enumerate(OFFSETS):
        slot = jnp.where(apart == offset, place, slot)
    far_at = cells + sender * CAP_FAR + position
    near_at = cells + devices * CAP_FAR + slot * EXTRA + position - CAP_FAR
    mapped = jnp.where(value < cells, value, jnp.where(position < CAP_FAR, far_at, near_at))
    for part in range(cells // LANES):
        index_out[pl.ds(part, kinds, stride=cells // LANES), :] = mapped[
            :, part * LANES : (part + 1) * LANES
        ]
    square[...] = jnp.zeros_like(square)
    for which in (0, 1):
        put_split(wd, which * PAIR, down_shift[:, which, :], square.at[which])
        put_split(ws, which * PAIR, sibling[:, which, :], square.at[2 + which])
    walked = None
    for depth in range(devices.bit_length() - 1):
        even = ((own[0] >> depth) & 1) == 0
        down = jnp.where(even, square[0], square[1])
        side = jnp.where(even, square[2], square[3])
        if walked is not None:
            high, low = halves(lanes([down, side]))
            both = bdot(lanes(tripled(walked)), rows([high, low, high]), NN)
            down, side = both[:, :LANES], both[:, LANES:]
        walked = down
        high, low = halves(side)
        path[:, depth * PAIR : (depth + 1) * PAIR] = lanes([high, low])
    starts = [0]
    for height in range(bits):
        starts.append(starts[-1] + (cells >> height))
    local = None
    for height in reversed(range(bits)):
        parts = []
        for which in (0, 1):
            total = None
            if local is not None:
                total = bdot(lanes(tripled(local)), weights(wd, which * PAIR), NT)
            if height >= 1:
                half = cells >> (height + 1)
                at = starts[height] + (1 - which) * half
                other = bdot(
                    lanes(tripled(agg[at : at + half, :])), weights(ws, which * PAIR), NT
                )
                total = other if total is None else total + other
            parts.append(total)
        local = rows(parts)
    local_out[...] = local


def near_kernel(own, slip_rows, low, high, lists, blocks, out, ext, columns):
    cells, elems = slip_rows.shape
    last = LANES - 1
    ext[...] = jnp.zeros_like(ext)
    ext[:HALO, :] = jnp.where(own[0] == 0, 0.0, low[3 * EXTRA :, :].astype(F32)).astype(BF16)
    ext[HALO : HALO + cells, :] = slip_rows[...]
    ext[HALO + cells : 2 * HALO + cells, :] = jnp.where(
        own[0] == last, 0.0, high[3 * EXTRA :, :].astype(F32)
    ).astype(BF16)
    columns[...] = jnp.zeros_like(columns)
    columns[: lists.shape[0], :] = lists[...].astype(F32)
    turned = columns[...].T
    at_lane = iota((cells, ext.shape[0]), 1).astype(F32)
    total = jnp.zeros((cells, elems), F32)
    for kind in range(NEAR):
        hot = one_hot(turned[:, kind : kind + 1], at_lane)
        gathered = bdot(hot, ext[...], NN).astype(BF16)
        total = total + bdot(gathered, blocks[kind], NT)
    out[...] = total.T


def top_levels(own, far, wu, wd, path, local_own, levels, coef, bits, tree_bits, result):
    devices = far.shape[0]
    spread = one_hot(iota((LANES, LANES), 0), iota((LANES, LANES), 1) % 4 + coef)
    keep = (iota((CAP_FAR, LANES), 1) // 4 == iota((CAP_FAR, LANES), 0)) & (
        iota((CAP_FAR, LANES), 1) < coef
    )
    found = []
    for first in range(0, devices, 16):
        part = bdot(far[first : first + 16].reshape(16 * CAP_FAR, LANES), spread, NN)
        part = jnp.where(keep[None], part.reshape(16, CAP_FAR, LANES), 0.0)
        found.append(jnp.sum(part, axis=1))
        yield
    level = bdot(bit_order(devices, tree_bits), rows(found).astype(BF16), NN)
    start, size = 0, devices
    starts = []
    for depth in range(tree_bits):
        levels[start : start + size, :] = level
        starts.append(start)
        start += size
        size //= 2
        if depth + 1 < tree_bits:
            stacked = lanes(tripled(level[:size]) + tripled(level[size:]))
            level = bdot(stacked, weights(wu, 0, PAIR), NT)
            yield
    others = []
    for depth in range(tree_bits):
        place = starts[depth] + reversed_bits((own[0] >> depth) ^ 1, tree_bits - depth)
        others += tripled(levels[pl.ds(place, 1), :])
    local = bdot(lanes(others), weights(path, *range(0, tree_bits * PAIR, PAIR)), NT)
    yield
    for _ in range(bits):
        stacked = lanes(tripled(local))
        local = rows([bdot(stacked, weights(wd, at), NT) for at in (0, PAIR)])
        yield
    cells = 1 << bits
    high, low = halves(local_own[...] + local)
    order = bit_order(cells, bits)
    result.append(bdot(order, high, NN) + bdot(order, low, NN))
    yield


def leaf_kernel(own, index_rows, far, low, high, plus, minus, mult, wu, wd, path,
                leaf_far, to_stress, local_own, near_part, out, index, arrived, table, levels, ts, *buffers):
    devices = far.shape[0]
    cells = mult.shape[0]
    coef = leaf_far.shape[1]
    bits = cells.bit_length() - 1
    tree_bits = devices.bit_length() - 1
    load = pltpu.make_async_copy(index_rows, index, arrived)
    load.start()
    ts[...] = jnp.zeros_like(ts)
    ts[:, :coef] = to_stress[...]
    table[:cells, :] = mult[...].astype(F32)
    step = 8
    for first in range(0, devices, step):
        table[cells + first * CAP_FAR : cells + (first + step) * CAP_FAR, :] = (
            far[first : first + step].reshape(step * CAP_FAR, LANES).astype(F32)
        )
    at = cells + devices * CAP_FAR
    for block in (low[:EXTRA, :], high[:EXTRA, :], plus[...], minus[...]):
        table[at : at + block.shape[0], :] = block.astype(F32)
        at += block.shape[0]

    load.wait()
    result = []
    tree = top_levels(
        own, far, wu, wd, path, local_own, levels, coef, bits, tree_bits, result
    )
    count = len(buffers)
    total = jnp.zeros((cells, coef), F32)
    for kind in range(TYPES):
        buffer = buffers[kind % count]
        for turn in range(cells):
            cell = reversed_bits(turn, bits)
            spot = kind * cells + cell
            row = index[spot // LANES, spot % LANES]
            buffer[cell : cell + 1, :] = table[pl.ds(row, 1), :]
        total = total + bdot(buffer[...].astype(BF16)[:, :coef], leaf_far[kind], NT)
        next(tree, None)
    total = total + result[0][:, :coef]
    out[...] = bdot(ts[:, :coef], total.astype(BF16), NT) + near_part[...]


def shape(dims, dtype):
    return jax.ShapeDtypeStruct(dims, dtype)


def kept(dims, dtype):
    return pltpu.VMEM(dims, dtype)


def held(x):
    return pltpu.with_memory_space_constraint(x, pltpu.VMEM)


def outer(x):
    return pltpu.with_memory_space_constraint(x, pltpu.HBM)


def limits(mib):
    return pltpu.CompilerParams(vmem_limit_bytes=mib << 20)


def scratch(dims, dtype):
    return pltpu.VMEM(dims, dtype)


def cost(flops):
    return pl.CostEstimate(flops=flops, bytes_accessed=10**6, transcendentals=0)


def shifted(block, by):
    count = lax.axis_size("leaf")
    return lax.ppermute(block, "leaf", [(i, (i + by) % count) for i in range(count)])


def body(
    slip,
    to_multipole,
    up_shift,
    down_shift,
    sibling_far,
    leaf_far,
    to_stress,
    near_blocks,
    send_cells,
    far_list,
    near_list,
):
    elems, cells = slip.shape
    devices = lax.axis_size("leaf")
    own = lax.axis_index("leaf").astype(jnp.int32).reshape(1)
    up_t, down_t, sibling_t = (
        jnp.transpose(w, (1, 0, 2)) for w in (up_shift, down_shift, sibling_far)
    )
    bundle = 3 * EXTRA + HALO
    far_send, up_send, down_send, plus_own, minus_own, mult, slip_rows, agg, wu = pl.pallas_call(
        send_kernel,
        out_shape=[
            shape((devices, CAP_FAR, LANES), BF16),
            kept((bundle, LANES), BF16),
            kept((bundle, LANES), BF16),
            kept((EXTRA, LANES), BF16),
            kept((EXTRA, LANES), BF16),
            kept((cells, LANES), BF16),
            kept((cells, elems), BF16),
            kept((2 * cells, LANES), F32),
            kept((LANES, 2 * PAIR), BF16),
        ],
        in_specs=[SM, VM, VM, VM, VM],
        out_specs=[pl.BlockSpec(memory_space=pl.ANY)] + [VM] * 8,
        scratch_shapes=[
            scratch((devices, CAP_FAR, LANES), BF16),
            pltpu.SemaphoreType.DMA((devices // GROUP,)),
            scratch((LANES, elems), BF16),
            scratch((devices, CAP_NEAR), F32),
            scratch((LANES, LANES), F32),
        ],
        compiler_params=limits(16),
        name="send",
    )(
        own,
        *(outer(x) for x in (slip, to_multipole, up_t, send_cells.reshape(devices, CAP_NEAR))),
    )
    low = shifted(up_send, 1)
    high = shifted(down_send, -1)
    far = lax.all_to_all(far_send, "leaf", split_axis=0, concat_axis=0, tiled=True)
    plus = shifted(rows([plus_own, low[EXTRA : 2 * EXTRA], high[2 * EXTRA : 3 * EXTRA]]), 3)
    minus = shifted(
        rows([minus_own, high[EXTRA : 2 * EXTRA], low[2 * EXTRA : 3 * EXTRA]]), -3
    )
    index_rows = (TYPES * cells // LANES + 7) // 8 * 8
    index, local_own, wd, path = pl.pallas_call(
        tree_kernel,
        out_shape=[
            kept((index_rows, LANES), jnp.int32),
            kept((cells, LANES), F32),
            kept((LANES, 2 * PAIR), BF16),
            kept((LANES, (devices.bit_length() - 1) * PAIR), BF16),
        ],
        in_specs=[SM, VM, VM, VM, VM],
        out_specs=[VM] * 4,
        scratch_shapes=[
            scratch((LANES, 2 * PAIR), BF16),
            scratch((4, LANES, LANES), F32),
        ],
        cost_estimate=cost(10**9),
        compiler_params=limits(16),
        name="tree",
    )(own, far_list, held(agg), down_t, sibling_t)
    near_part = pl.pallas_call(
        near_kernel,
        out_shape=kept((elems, cells), F32),
        in_specs=[SM] + [VM] * 5,
        out_specs=VM,
        scratch_shapes=[
            scratch((cells + LANES, elems), BF16),
            scratch((LANES, cells), F32),
        ],
        cost_estimate=cost(10**9),
        compiler_params=limits(16),
        name="near",
    )(own, held(slip_rows), held(low), held(high), near_list, held(near_blocks))
    table_rows = cells + devices * CAP_FAR + len(OFFSETS) * EXTRA
    return pl.pallas_call(
        leaf_kernel,
        out_shape=shape((elems, cells), F32),
        in_specs=[SM] + [VM] * 10 + [VM] * 4,
        out_specs=VM,
        scratch_shapes=[
            pltpu.SMEM((index_rows, LANES), jnp.int32),
            pltpu.SemaphoreType.DMA,
            scratch((table_rows, LANES), F32),
            scratch((2 * devices, LANES), F32),
            scratch((elems, LANES), BF16),
        ]
        + [scratch((cells, LANES), F32)] * 6,
        compiler_params=limits(24),
        name="leaf",
    )(
        own,
        held(index),
        held(far),
        held(low),
        held(high),
        held(plus),
        held(minus),
        held(mult),
        held(wu),
        held(wd),
        held(path),
        held(leaf_far),
        held(to_stress),
        held(local_own),
        held(near_part),
    )


def solution(mesh):
    return jax.shard_map(
        body,
        mesh=mesh,
        in_specs=(
            P(None, "leaf"),
            P(),
            P(),
            P(),
            P(),
            P(),
            P(),
            P(),
            P("leaf", None),
            P(None, "leaf"),
            P(None, "leaf"),
        ),
        out_specs=P(None, "leaf"),
        check_vma=False,
    )
```

```python
import jax
import jax.numpy as jnp
from jax import lax
from jax.experimental import pallas as pl
from jax.experimental.pallas import tpu as pltpu
from jax.sharding import PartitionSpec as P


NEAR = 9
TYPES = 27
HALO = 32
CAP_NEAR = 128
CAP_FAR = 32
EXTRA = CAP_NEAR - CAP_FAR
LANES = 128
PAIR = 2 * LANES
GROUP = 8
MIX = 100
SLACK = 8
OFFSETS = (-1, 1, -3, -4, -2, 3, 4, 2)

VM = pl.BlockSpec(memory_space=pltpu.VMEM)
SM = pl.BlockSpec(memory_space=pltpu.SMEM)
F32 = jnp.float32
BF16 = jnp.bfloat16
NT = (((1,), (1,)), ((), ()))
NN = (((1,), (0,)), ((), ()))


def iota(dims, dim):
    return lax.broadcasted_iota(jnp.int32, dims, dim)


def reversed_bits(value, bits):
    out = 0
    for bit in range(bits):
        out = out | ((value >> bit) & 1) << (bits - 1 - bit)
    return out


def bdot(a, b, dims):
    return lax.dot_general(a, b, dims, preferred_element_type=F32)


def one_hot(column, row):
    return jnp.where(column == row, 1.0, 0.0).astype(BF16)


def halves(x):
    high = x.astype(BF16)
    return high, (x - high.astype(F32)).astype(BF16)


def tripled(x):
    high, low = halves(x)
    return [high, high, low]


def lanes(parts):
    return jnp.concatenate(parts, axis=1)


def rows(parts):
    return jnp.concatenate(parts, axis=0)


def put_split(ref, at, block, square):
    square[: block.shape[0], : block.shape[1]] = block
    high, low = halves(square[...])
    ref[:, at : at + LANES] = high
    ref[:, at + LANES : at + PAIR] = low


def weights(ref, *starts):
    parts = []
    for at in starts:
        high = ref[:, at : at + LANES]
        parts += [high, ref[:, at + LANES : at + PAIR], high]
    return lanes(parts)


def bit_order(size, bits):
    inner = reversed_bits(iota((8, size), 0), 3) << (bits - 3)
    gap = iota((8, size), 1) - inner
    blocks = [
        jnp.where(gap == reversed_bits(block, bits - 3), 1.0, 0.0) for block in range(size // 8)
    ]
    return rows(blocks).astype(BF16)


def matches(picked, spare, cells):
    at = iota((LANES, cells), 0)
    return jnp.where(
        at == spare, -iota((LANES, cells), 1).astype(F32), jnp.where(picked(at), 1.0, 0.0)
    ).astype(BF16)


def send_kernel(own, slip, to_mult, up_shift, send, far_hbm, up_out, down_out, plus_out,
                minus_out, mult_out, slip_out, agg_out, wu, far_out, sent, tm,
                lists, square):
    cells = slip.shape[1]
    coef = to_mult.shape[0]
    devices = send.shape[0]
    bits = cells.bit_length() - 1
    tm[...] = jnp.zeros_like(tm)
    tm[:coef, :] = to_mult[...]
    square[...] = jnp.zeros_like(square)
    put_split(wu, 0, up_shift[:, 0, :], square)
    put_split(wu, PAIR, up_shift[:, 1, :], square)
    unit = one_hot(iota((cells, cells), 0), iota((cells, cells), 1))
    slip_rows = bdot(unit, slip[...], NT).astype(BF16)
    slip_out[...] = slip_rows
    mult = bdot(slip_rows, tm[...], NT).astype(BF16)
    mult_out[...] = mult
    lists[:devices, :] = send[...].astype(F32)
    level = bdot(bit_order(cells, bits), mult, NN)
    start, size = 0, cells
    for _ in range(bits):
        agg_out[start : start + size, :] = level
        start += size
        size //= 2
        level = bdot(
            lanes(tripled(level[:size]) + tripled(level[size:])), weights(wu, 0, PAIR), NT
        )
    spread = one_hot(iota((LANES, LANES), 0) % 4 + coef, iota((LANES, LANES), 1))
    own_row = (iota((CAP_FAR, LANES), 1) // 4) == iota((CAP_FAR, LANES), 0)
    placed = jnp.where(own_row, level, 0.0).astype(BF16)
    tail = rows([bdot(placed, spread, NN)] * GROUP)
    lane = iota((CAP_FAR, LANES), 1)
    own_slot = lane == iota((CAP_FAR, LANES), 0)
    rest = jnp.where(lane == CAP_FAR, 1.0, 0.0)
    far_match = matches(lambda at: at < CAP_FAR, CAP_FAR, cells)
    cell_row = iota((CAP_FAR, cells), 1).astype(F32)
    turned = lists[:devices, :].T
    copies = []
    for first in range(0, devices, GROUP):
        group = range(first, first + GROUP)
        if first // GROUP % MIX == 0:
            hot = rows([one_hot(turned[:CAP_FAR, d : d + 1], cell_row) for d in group])
        else:
            spots = rows([jnp.where(own_slot, lists[d : d + 1, :], rest) for d in group])
            hot = one_hot(bdot(spots.astype(BF16), far_match, NN), 0.0)
        far_out[first : first + GROUP] = (
            (bdot(hot, mult, NN) + tail).astype(BF16).reshape(GROUP, CAP_FAR, LANES)
        )
        copies.append(
            pltpu.make_async_copy(
                far_out.at[pl.ds(first, GROUP)],
                far_hbm.at[pl.ds(first, GROUP)],
                sent.at[first // GROUP],
            )
        )
        copies[-1].start()
    lane = iota((EXTRA, LANES), 1)
    own_slot = lane == iota((EXTRA, LANES), 0) + CAP_FAR
    rest = jnp.where(lane == 0, 1.0, 0.0)
    near_match = matches(lambda at: at >= CAP_FAR, 0, cells)
    homes = [(up_out, 0, 1), (up_out, 1, 4), (up_out, 2, -2), (down_out, 0, -1),
             (down_out, 1, -4), (down_out, 2, 2), (plus_out, 0, 3), (minus_out, 0, -3)]
    for ref, place, step in homes:
        dest = (own[0] + step) & (devices - 1)
        spots = jnp.where(own_slot, lists[pl.ds(dest, 1), :], rest).astype(BF16)
        hot = one_hot(bdot(spots, near_match, NN), 0.0)
        ref[place * EXTRA : (place + 1) * EXTRA, :] = bdot(hot, mult, NN).astype(BF16)
    up_out[3 * EXTRA :, :] = slip_rows[cells - HALO :]
    down_out[3 * EXTRA :, :] = slip_rows[:HALO]
    for copy in copies:
        copy.wait()


def tree_kernel(own, far_list, agg, down_shift, sibling, index_out, local_out, wd, path, ws,
                square):
    cells = far_list.shape[1]
    kinds = far_list.shape[0]
    bits = cells.bit_length() - 1
    devices = LANES
    value = far_list[...]
    relative = value - cells
    sender = relative >> 7
    position = relative & (CAP_NEAR - 1)
    apart = sender - own[0]
    slot = jnp.zeros_like(value)
    for place, offset in enumerate(OFFSETS):
        slot = jnp.where(apart == offset, place, slot)
    far_at = cells + sender * CAP_FAR + position
    near_at = cells + devices * CAP_FAR + slot * EXTRA + position - CAP_FAR
    mapped = jnp.where(value < cells, value, jnp.where(position < CAP_FAR, far_at, near_at))
    for part in range(cells // LANES):
        index_out[pl.ds(part, kinds, stride=cells // LANES), :] = mapped[
            :, part * LANES : (part + 1) * LANES
        ]
    square[...] = jnp.zeros_like(square)
    for which in (0, 1):
        put_split(wd, which * PAIR, down_shift[:, which, :], square.at[which])
        put_split(ws, which * PAIR, sibling[:, which, :], square.at[2 + which])
    walked = None
    for depth in range(devices.bit_length() - 1):
        even = ((own[0] >> depth) & 1) == 0
        down = jnp.where(even, square[0], square[1])
        side = jnp.where(even, square[2], square[3])
        if walked is not None:
            high, low = halves(lanes([down, side]))
            both = bdot(lanes(tripled(walked)), rows([high, low, high]), NN)
            down, side = both[:, :LANES], both[:, LANES:]
        walked = down
        high, low = halves(side)
        path[:, depth * PAIR : (depth + 1) * PAIR] = lanes([high, low])
    starts = [0]
    for height in range(bits):
        starts.append(starts[-1] + (cells >> height))
    local = None
    for height in reversed(range(bits)):
        parts = []
        for which in (0, 1):
            total = None
            if local is not None:
                total = bdot(lanes(tripled(local)), weights(wd, which * PAIR), NT)
            if height >= 1:
                half = cells >> (height + 1)
                at = starts[height] + (1 - which) * half
                other = bdot(
                    lanes(tripled(agg[at : at + half, :])), weights(ws, which * PAIR), NT
                )
                total = other if total is None else total + other
            parts.append(total)
        local = rows(parts)
    local_out[...] = local


def near_kernel(own, slip_rows, low, high, lists, blocks, out, ext, columns):
    cells, elems = slip_rows.shape
    last = LANES - 1
    ext[...] = jnp.zeros_like(ext)
    ext[:HALO, :] = jnp.where(own[0] == 0, 0.0, low[3 * EXTRA :, :].astype(F32)).astype(BF16)
    ext[HALO : HALO + cells, :] = slip_rows[...]
    ext[HALO + cells : 2 * HALO + cells, :] = jnp.where(
        own[0] == last, 0.0, high[3 * EXTRA :, :].astype(F32)
    ).astype(BF16)
    columns[...] = jnp.zeros_like(columns)
    columns[: lists.shape[0], :] = lists[...].astype(F32)
    turned = columns[...].T
    at_lane = iota((cells, ext.shape[0]), 1).astype(F32)
    total = jnp.zeros((cells, elems), F32)
    for kind in range(NEAR):
        hot = one_hot(turned[:, kind : kind + 1], at_lane)
        gathered = bdot(hot, ext[...], NN).astype(BF16)
        total = total + bdot(gathered, blocks[kind], NT)
    out[...] = total.T


def top_levels(own, far, wu, wd, path, local_own, levels, coef, bits, tree_bits, result):
    devices = far.shape[0]
    spread = one_hot(iota((LANES, LANES), 0), iota((LANES, LANES), 1) % 4 + coef)
    keep = (iota((CAP_FAR, LANES), 1) // 4 == iota((CAP_FAR, LANES), 0)) & (
        iota((CAP_FAR, LANES), 1) < coef
    )
    found = []
    for first in range(0, devices, 16):
        part = bdot(far[first : first + 16].reshape(16 * CAP_FAR, LANES), spread, NN)
        part = jnp.where(keep[None], part.reshape(16, CAP_FAR, LANES), 0.0)
        found.append(jnp.sum(part, axis=1))
        yield
    level = bdot(bit_order(devices, tree_bits), rows(found).astype(BF16), NN)
    start, size = 0, devices
    starts = []
    for depth in range(tree_bits):
        levels[start : start + size, :] = level
        starts.append(start)
        start += size
        size //= 2
        if depth + 1 < tree_bits:
            stacked = lanes(tripled(level[:size]) + tripled(level[size:]))
            level = bdot(stacked, weights(wu, 0, PAIR), NT)
            yield
    others = []
    for depth in range(tree_bits):
        place = starts[depth] + reversed_bits((own[0] >> depth) ^ 1, tree_bits - depth)
        others += tripled(levels[pl.ds(place, 1), :])
    local = bdot(lanes(others), weights(path, *range(0, tree_bits * PAIR, PAIR)), NT)
    yield
    for _ in range(bits):
        stacked = lanes(tripled(local))
        local = rows([bdot(stacked, weights(wd, at), NT) for at in (0, PAIR)])
        yield
    cells = 1 << bits
    high, low = halves(local_own[...] + local)
    order = bit_order(cells, bits)
    result.append(bdot(order, high, NN) + bdot(order, low, NN))
    yield


def leaf_kernel(own, index_rows, far, low, high, plus, minus, mult, wu, wd, path,
                leaf_far, to_stress, local_own, near_part, out, index, arrived, table, levels, ts, *buffers):
    devices = far.shape[0]
    cells = mult.shape[0]
    coef = leaf_far.shape[1]
    bits = cells.bit_length() - 1
    tree_bits = devices.bit_length() - 1
    load = pltpu.make_async_copy(index_rows, index, arrived)
    load.start()
    ts[...] = jnp.zeros_like(ts)
    ts[:, :coef] = to_stress[...]
    table[:cells, :] = mult[...].astype(F32)
    step = 8
    for first in range(0, devices, step):
        table[cells + first * CAP_FAR : cells + (first + step) * CAP_FAR, :] = (
            far[first : first + step].reshape(step * CAP_FAR, LANES).astype(F32)
        )
    at = cells + devices * CAP_FAR
    for block in (low[:EXTRA, :], high[:EXTRA, :], plus[...], minus[...]):
        table[at : at + block.shape[0], :] = block.astype(F32)
        at += block.shape[0]

    load.wait()
    result = []
    tree = top_levels(
        own, far, wu, wd, path, local_own, levels, coef, bits, tree_bits, result
    )
    count = len(buffers)
    total = jnp.zeros((cells, coef), F32)
    for kind in range(TYPES):
        buffer = buffers[kind % count]
        for turn in range(cells):
            cell = reversed_bits(turn, bits)
            spot = kind * cells + cell
            row = index[spot // LANES, spot % LANES]
            buffer[cell : cell + 1, :] = table[pl.ds(row, 1), :]
        total = total + bdot(buffer[:cells, :].astype(BF16)[:, :coef], leaf_far[kind], NT)
        next(tree, None)
    total = total + result[0][:, :coef]
    out[...] = bdot(ts[:, :coef], total.astype(BF16), NT) + near_part[...]


def shape(dims, dtype):
    return jax.ShapeDtypeStruct(dims, dtype)


def kept(dims, dtype):
    return pltpu.VMEM(dims, dtype)


def held(x):
    return pltpu.with_memory_space_constraint(x, pltpu.VMEM)


def outer(x):
    return pltpu.with_memory_space_constraint(x, pltpu.HBM)


def limits(mib):
    return pltpu.CompilerParams(vmem_limit_bytes=mib << 20)


def scratch(dims, dtype):
    return pltpu.VMEM(dims, dtype)


def cost(flops):
    return pl.CostEstimate(flops=flops, bytes_accessed=10**6, transcendentals=0)


def shifted(block, by):
    count = lax.axis_size("leaf")
    return lax.ppermute(block, "leaf", [(i, (i + by) % count) for i in range(count)])


def body(
    slip,
    to_multipole,
    up_shift,
    down_shift,
    sibling_far,
    leaf_far,
    to_stress,
    near_blocks,
    send_cells,
    far_list,
    near_list,
):
    elems, cells = slip.shape
    devices = lax.axis_size("leaf")
    own = lax.axis_index("leaf").astype(jnp.int32).reshape(1)
    up_t, down_t, sibling_t = (
        jnp.transpose(w, (1, 0, 2)) for w in (up_shift, down_shift, sibling_far)
    )
    bundle = 3 * EXTRA + HALO
    far_send, up_send, down_send, plus_own, minus_own, mult, slip_rows, agg, wu = pl.pallas_call(
        send_kernel,
        out_shape=[
            shape((devices, CAP_FAR, LANES), BF16),
            kept((bundle, LANES), BF16),
            kept((bundle, LANES), BF16),
            kept((EXTRA, LANES), BF16),
            kept((EXTRA, LANES), BF16),
            kept((cells, LANES), BF16),
            kept((cells, elems), BF16),
            kept((2 * cells + SLACK, LANES), F32),
            kept((LANES, 2 * PAIR), BF16),
        ],
        in_specs=[SM, VM, VM, VM, VM],
        out_specs=[pl.BlockSpec(memory_space=pl.ANY)] + [VM] * 8,
        scratch_shapes=[
            scratch((devices, CAP_FAR, LANES), BF16),
            pltpu.SemaphoreType.DMA((devices // GROUP,)),
            scratch((LANES, elems), BF16),
            scratch((devices + SLACK, CAP_NEAR), F32),
            scratch((LANES, LANES), F32),
        ],
        compiler_params=limits(16),
        name="send",
    )(
        own,
        *(outer(x) for x in (slip, to_multipole, up_t, send_cells.reshape(devices, CAP_NEAR))),
    )
    low = shifted(up_send, 1)
    high = shifted(down_send, -1)
    far = lax.all_to_all(far_send, "leaf", split_axis=0, concat_axis=0, tiled=True)
    plus = shifted(rows([plus_own, low[EXTRA : 2 * EXTRA], high[2 * EXTRA : 3 * EXTRA]]), 3)
    minus = shifted(
        rows([minus_own, high[EXTRA : 2 * EXTRA], low[2 * EXTRA : 3 * EXTRA]]), -3
    )
    index_rows = cells // LANES * ((TYPES + 7) // 8 * 8)
    index, local_own, wd, path = pl.pallas_call(
        tree_kernel,
        out_shape=[
            kept((index_rows, LANES), jnp.int32),
            kept((cells, LANES), F32),
            kept((LANES, 2 * PAIR), BF16),
            kept((LANES, (devices.bit_length() - 1) * PAIR), BF16),
        ],
        in_specs=[SM, VM, VM, VM, VM],
        out_specs=[VM] * 4,
        scratch_shapes=[
            scratch((LANES, 2 * PAIR), BF16),
            scratch((4, LANES, LANES), F32),
        ],
        cost_estimate=cost(10**9),
        compiler_params=limits(16),
        name="tree",
    )(own, far_list, held(agg), down_t, sibling_t)
    near_part = pl.pallas_call(
        near_kernel,
        out_shape=kept((elems, cells), F32),
        in_specs=[SM] + [VM] * 5,
        out_specs=VM,
        scratch_shapes=[
            scratch((cells + LANES, elems), BF16),
            scratch((LANES, cells), F32),
        ],
        cost_estimate=cost(10**9),
        compiler_params=limits(16),
        name="near",
    )(own, held(slip_rows), held(low), held(high), near_list, held(near_blocks))
    table_rows = cells + devices * CAP_FAR + len(OFFSETS) * EXTRA
    return pl.pallas_call(
        leaf_kernel,
        out_shape=shape((elems, cells), F32),
        in_specs=[SM] + [VM] * 10 + [VM] * 4,
        out_specs=VM,
        scratch_shapes=[
            pltpu.SMEM((index_rows, LANES), jnp.int32),
            pltpu.SemaphoreType.DMA,
            scratch((table_rows + SLACK, LANES), F32),
            scratch((2 * devices + SLACK, LANES), F32),
            scratch((elems, LANES), BF16),
        ]
        + [scratch((cells + SLACK, LANES), F32)] * 6,
        compiler_params=limits(24),
        name="leaf",
    )(
        own,
        held(index),
        held(far),
        held(low),
        held(high),
        held(plus),
        held(minus),
        held(mult),
        held(wu),
        held(wd),
        held(path),
        held(leaf_far),
        held(to_stress),
        held(local_own),
        held(near_part),
    )


def solution(mesh):
    return jax.shard_map(
        body,
        mesh=mesh,
        in_specs=(
            P(None, "leaf"),
            P(),
            P(),
            P(),
            P(),
            P(),
            P(),
            P(),
            P("leaf", None),
            P(None, "leaf"),
            P(None, "leaf"),
        ),
        out_specs=P(None, "leaf"),
        check_vma=False,
    )
```

```python
import jax
import jax.numpy as jnp
from jax import lax
from jax.experimental import pallas as pl
from jax.experimental.pallas import tpu as pltpu
from jax.sharding import PartitionSpec as P


NEAR = 9
TYPES = 27
HALO = 32
CAP_NEAR = 128
CAP_FAR = 32
EXTRA = CAP_NEAR - CAP_FAR
LANES = 128
PAIR = 2 * LANES
GROUP = 8
OFFSETS = (-1, 1, -3, -4, -2, 3, 4, 2)

VM = pl.BlockSpec(memory_space=pltpu.VMEM)
SM = pl.BlockSpec(memory_space=pltpu.SMEM)
F32 = jnp.float32
BF16 = jnp.bfloat16
NT = (((1,), (1,)), ((), ()))
NN = (((1,), (0,)), ((), ()))


def iota(dims, dim):
    return lax.broadcasted_iota(jnp.int32, dims, dim)


def reversed_bits(value, bits):
    out = 0
    for bit in range(bits):
        out = out | ((value >> bit) & 1) << (bits - 1 - bit)
    return out


def bdot(a, b, dims):
    return lax.dot_general(a, b, dims, preferred_element_type=F32)


def one_hot(column, row):
    return jnp.where(column == row, 1.0, 0.0).astype(BF16)


def halves(x):
    high = x.astype(BF16)
    return high, (x - high.astype(F32)).astype(BF16)


def tripled(x):
    high, low = halves(x)
    return [high, high, low]


def lanes(parts):
    return jnp.concatenate(parts, axis=1)


def rows(parts):
    return jnp.concatenate(parts, axis=0)


def put_split(ref, at, block, square):
    square[: block.shape[0], : block.shape[1]] = block
    high, low = halves(square[...])
    ref[:, at : at + LANES] = high
    ref[:, at + LANES : at + PAIR] = low


def weights(ref, *starts):
    parts = []
    for at in starts:
        high = ref[:, at : at + LANES]
        parts += [high, ref[:, at + LANES : at + PAIR], high]
    return lanes(parts)


def bit_order(size, bits):
    inner = reversed_bits(iota((8, size), 0), 3) << (bits - 3)
    gap = iota((8, size), 1) - inner
    blocks = [
        jnp.where(gap == reversed_bits(block, bits - 3), 1.0, 0.0) for block in range(size // 8)
    ]
    return rows(blocks).astype(BF16)


def matches(picked, spare, cells):
    at = iota((LANES, cells), 0)
    return jnp.where(
        at == spare, -iota((LANES, cells), 1).astype(F32), jnp.where(picked(at), 1.0, 0.0)
    ).astype(BF16)


def send_kernel(own, slip, to_mult, up_shift, send, far_hbm, up_out, down_out, plus_out,
                minus_out, mult_out, slip_out, agg_out, wu, far_out, sent, tm,
                lists, square):
    cells = slip.shape[1]
    coef = to_mult.shape[0]
    devices = send.shape[0]
    bits = cells.bit_length() - 1
    tm[...] = jnp.zeros_like(tm)
    tm[:coef, :] = to_mult[...]
    square[...] = jnp.zeros_like(square)
    put_split(wu, 0, up_shift[:, 0, :], square)
    put_split(wu, PAIR, up_shift[:, 1, :], square)
    unit = one_hot(iota((cells, cells), 0), iota((cells, cells), 1))
    slip_rows = bdot(unit, slip[...], NT).astype(BF16)
    slip_out[...] = slip_rows
    mult = bdot(slip_rows, tm[...], NT).astype(BF16)
    mult_out[...] = mult
    lists[...] = send[...].astype(F32)
    level = bdot(bit_order(cells, bits), mult, NN)
    start, size = 0, cells
    for _ in range(bits):
        agg_out[start : start + size, :] = level
        start += size
        size //= 2
        level = bdot(
            lanes(tripled(level[:size]) + tripled(level[size:])), weights(wu, 0, PAIR), NT
        )
    spread = one_hot(iota((LANES, LANES), 0) % 4 + coef, iota((LANES, LANES), 1))
    own_row = (iota((CAP_FAR, LANES), 1) // 4) == iota((CAP_FAR, LANES), 0)
    placed = jnp.where(own_row, level, 0.0).astype(BF16)
    tail = rows([bdot(placed, spread, NN)] * GROUP)
    lane = iota((CAP_FAR, LANES), 1)
    own_slot = lane == iota((CAP_FAR, LANES), 0)
    rest = jnp.where(lane == CAP_FAR, 1.0, 0.0)
    far_match = matches(lambda at: at < CAP_FAR, CAP_FAR, cells)
    copies = []
    for first in range(0, devices, GROUP):
        group = range(first, first + GROUP)
        spots = rows([jnp.where(own_slot, lists[d : d + 1, :], rest) for d in group])
        hot = one_hot(bdot(spots.astype(BF16), far_match, NN), 0.0)
        far_out[first : first + GROUP] = (
            (bdot(hot, mult, NN) + tail).astype(BF16).reshape(GROUP, CAP_FAR, LANES)
        )
        copies.append(
            pltpu.make_async_copy(
                far_out.at[pl.ds(first, GROUP)],
                far_hbm.at[pl.ds(first, GROUP)],
                sent.at[first // GROUP],
            )
        )
        copies[-1].start()
    lane = iota((EXTRA, LANES), 1)
    own_slot = lane == iota((EXTRA, LANES), 0) + CAP_FAR
    rest = jnp.where(lane == 0, 1.0, 0.0)
    near_match = matches(lambda at: at >= CAP_FAR, 0, cells)
    homes = [(up_out, 0, 1), (up_out, 1, 4), (up_out, 2, -2), (down_out, 0, -1),
             (down_out, 1, -4), (down_out, 2, 2), (plus_out, 0, 3), (minus_out, 0, -3)]
    for ref, place, step in homes:
        dest = (own[0] + step) & (devices - 1)
        spots = jnp.where(own_slot, lists[pl.ds(dest, 1), :], rest).astype(BF16)
        hot = one_hot(bdot(spots, near_match, NN), 0.0)
        ref[place * EXTRA : (place + 1) * EXTRA, :] = bdot(hot, mult, NN).astype(BF16)
    up_out[3 * EXTRA :, :] = slip_rows[cells - HALO :]
    down_out[3 * EXTRA :, :] = slip_rows[:HALO]
    for copy in copies:
        copy.wait()


def tree_kernel(own, far_list, agg, down_shift, sibling, index_out, local_out, wd, path, ws,
                square):
    cells = far_list.shape[1]
    kinds = far_list.shape[0]
    bits = cells.bit_length() - 1
    devices = LANES
    value = far_list[...]
    relative = value - cells
    sender = relative >> 7
    position = relative & (CAP_NEAR - 1)
    apart = sender - own[0]
    slot = jnp.zeros_like(value)
    for place, offset in enumerate(OFFSETS):
        slot = jnp.where(apart == offset, place, slot)
    far_at = cells + sender * CAP_FAR + position
    near_at = cells + devices * CAP_FAR + slot * EXTRA + position - CAP_FAR
    mapped = jnp.where(value < cells, value, jnp.where(position < CAP_FAR, far_at, near_at))
    for part in range(cells // LANES):
        index_out[pl.ds(part, kinds, stride=cells // LANES), :] = mapped[
            :, part * LANES : (part + 1) * LANES
        ]
    square[...] = jnp.zeros_like(square)
    for which in (0, 1):
        put_split(wd, which * PAIR, down_shift[:, which, :], square.at[which])
        put_split(ws, which * PAIR, sibling[:, which, :], square.at[2 + which])
    walked = None
    for depth in range(devices.bit_length() - 1):
        even = ((own[0] >> depth) & 1) == 0
        down = jnp.where(even, square[0], square[1])
        side = jnp.where(even, square[2], square[3])
        if walked is not None:
            high, low = halves(lanes([down, side]))
            both = bdot(lanes(tripled(walked)), rows([high, low, high]), NN)
            down, side = both[:, :LANES], both[:, LANES:]
        walked = down
        high, low = halves(side)
        path[:, depth * PAIR : (depth + 1) * PAIR] = lanes([high, low])
    starts = [0]
    for height in range(bits):
        starts.append(starts[-1] + (cells >> height))
    local = None
    for height in reversed(range(bits)):
        parts = []
        for which in (0, 1):
            total = None
            if local is not None:
                total = bdot(lanes(tripled(local)), weights(wd, which * PAIR), NT)
            if height >= 1:
                half = cells >> (height + 1)
                at = starts[height] + (1 - which) * half
                other = bdot(
                    lanes(tripled(agg[at : at + half, :])), weights(ws, which * PAIR), NT
                )
                total = other if total is None else total + other
            parts.append(total)
        local = rows(parts)
    local_out[...] = local


def near_kernel(own, slip_rows, low, high, lists, blocks, out, ext, columns):
    cells, elems = slip_rows.shape
    last = LANES - 1
    ext[...] = jnp.zeros_like(ext)
    ext[:HALO, :] = jnp.where(own[0] == 0, 0.0, low[3 * EXTRA :, :].astype(F32)).astype(BF16)
    ext[HALO : HALO + cells, :] = slip_rows[...]
    ext[HALO + cells : 2 * HALO + cells, :] = jnp.where(
        own[0] == last, 0.0, high[3 * EXTRA :, :].astype(F32)
    ).astype(BF16)
    columns[...] = jnp.zeros_like(columns)
    columns[: lists.shape[0], :] = lists[...].astype(F32)
    turned = columns[...].T
    at_lane = iota((cells, ext.shape[0]), 1).astype(F32)
    total = jnp.zeros((cells, elems), F32)
    for kind in range(NEAR):
        hot = one_hot(turned[:, kind : kind + 1], at_lane)
        gathered = bdot(hot, ext[...], NN).astype(BF16)
        total = total + bdot(gathered, blocks[kind], NT)
    out[...] = total.T


def top_levels(own, far, wu, wd, path, local_own, levels, coef, bits, tree_bits, result):
    devices = far.shape[0]
    spread = one_hot(iota((LANES, LANES), 0), iota((LANES, LANES), 1) % 4 + coef)
    keep = (iota((CAP_FAR, LANES), 1) // 4 == iota((CAP_FAR, LANES), 0)) & (
        iota((CAP_FAR, LANES), 1) < coef
    )
    found = []
    for first in range(0, devices, 16):
        part = bdot(far[first : first + 16].reshape(16 * CAP_FAR, LANES), spread, NN)
        part = jnp.where(keep[None], part.reshape(16, CAP_FAR, LANES), 0.0)
        found.append(jnp.sum(part, axis=1))
        yield
    level = bdot(bit_order(devices, tree_bits), rows(found).astype(BF16), NN)
    start, size = 0, devices
    starts = []
    for depth in range(tree_bits):
        levels[start : start + size, :] = level
        starts.append(start)
        start += size
        size //= 2
        if depth + 1 < tree_bits:
            stacked = lanes(tripled(level[:size]) + tripled(level[size:]))
            level = bdot(stacked, weights(wu, 0, PAIR), NT)
            yield
    others = []
    for depth in range(tree_bits):
        place = starts[depth] + reversed_bits((own[0] >> depth) ^ 1, tree_bits - depth)
        others += tripled(levels[pl.ds(place, 1), :])
    local = bdot(lanes(others), weights(path, *range(0, tree_bits * PAIR, PAIR)), NT)
    yield
    for _ in range(bits):
        stacked = lanes(tripled(local))
        local = rows([bdot(stacked, weights(wd, at), NT) for at in (0, PAIR)])
        yield
    cells = 1 << bits
    high, low = halves(local_own[...] + local)
    order = bit_order(cells, bits)
    result.append(bdot(order, high, NN) + bdot(order, low, NN))
    yield


def leaf_kernel(own, index_rows, far, low, high, plus, minus, mult, wu, wd, path,
                leaf_far, to_stress, local_own, near_part, out, index, arrived, table, levels, ts, *buffers):
    devices = far.shape[0]
    cells = mult.shape[0]
    coef = leaf_far.shape[1]
    bits = cells.bit_length() - 1
    tree_bits = devices.bit_length() - 1
    load = pltpu.make_async_copy(index_rows, index, arrived)
    load.start()
    ts[...] = jnp.zeros_like(ts)
    ts[:, :coef] = to_stress[...]
    table[:cells, :] = mult[...].astype(F32)
    step = 8
    for first in range(0, devices, step):
        table[cells + first * CAP_FAR : cells + (first + step) * CAP_FAR, :] = (
            far[first : first + step].reshape(step * CAP_FAR, LANES).astype(F32)
        )
    at = cells + devices * CAP_FAR
    for block in (low[:EXTRA, :], high[:EXTRA, :], plus[...], minus[...]):
        table[at : at + block.shape[0], :] = block.astype(F32)
        at += block.shape[0]

    load.wait()
    result = []
    tree = top_levels(
        own, far, wu, wd, path, local_own, levels, coef, bits, tree_bits, result
    )
    count = len(buffers)
    total = jnp.zeros((cells, coef), F32)
    for kind in range(TYPES):
        buffer = buffers[kind % count]
        for turn in range(cells):
            cell = reversed_bits(turn, bits)
            spot = kind * cells + cell
            row = index[spot // LANES, spot % LANES]
            buffer[cell : cell + 1, :] = table[pl.ds(row, 1), :]
        total = total + bdot(buffer[...].astype(BF16)[:, :coef], leaf_far[kind], NT)
        next(tree, None)
        if result:
            total = total + result.pop()[:, :coef]
    out[...] = bdot(ts[:, :coef], total.astype(BF16), NT) + near_part[...]


def shape(dims, dtype):
    return jax.ShapeDtypeStruct(dims, dtype)


def kept(dims, dtype):
    return pltpu.VMEM(dims, dtype)


def held(x):
    return pltpu.with_memory_space_constraint(x, pltpu.VMEM)


def outer(x):
    return pltpu.with_memory_space_constraint(x, pltpu.HBM)


def limits(mib):
    return pltpu.CompilerParams(vmem_limit_bytes=mib << 20)


def scratch(dims, dtype):
    return pltpu.VMEM(dims, dtype)


def cost(flops):
    return pl.CostEstimate(flops=flops, bytes_accessed=10**6, transcendentals=0)


def shifted(block, by):
    count = lax.axis_size("leaf")
    return lax.ppermute(block, "leaf", [(i, (i + by) % count) for i in range(count)])


def body(
    slip,
    to_multipole,
    up_shift,
    down_shift,
    sibling_far,
    leaf_far,
    to_stress,
    near_blocks,
    send_cells,
    far_list,
    near_list,
):
    elems, cells = slip.shape
    devices = lax.axis_size("leaf")
    own = lax.axis_index("leaf").astype(jnp.int32).reshape(1)
    up_t, down_t, sibling_t = (
        jnp.transpose(w, (1, 0, 2)) for w in (up_shift, down_shift, sibling_far)
    )
    bundle = 3 * EXTRA + HALO
    far_send, up_send, down_send, plus_own, minus_own, mult, slip_rows, agg, wu = pl.pallas_call(
        send_kernel,
        out_shape=[
            shape((devices, CAP_FAR, LANES), BF16),
            kept((bundle, LANES), BF16),
            kept((bundle, LANES), BF16),
            kept((EXTRA, LANES), BF16),
            kept((EXTRA, LANES), BF16),
            kept((cells, LANES), BF16),
            kept((cells, elems), BF16),
            kept((2 * cells, LANES), F32),
            kept((LANES, 2 * PAIR), BF16),
        ],
        in_specs=[SM, VM, VM, VM, VM],
        out_specs=[pl.BlockSpec(memory_space=pl.ANY)] + [VM] * 8,
        scratch_shapes=[
            scratch((devices, CAP_FAR, LANES), BF16),
            pltpu.SemaphoreType.DMA((devices // GROUP,)),
            scratch((LANES, elems), BF16),
            scratch((devices, CAP_NEAR), F32),
            scratch((LANES, LANES), F32),
        ],
        compiler_params=limits(16),
        name="send",
    )(
        own,
        *(outer(x) for x in (slip, to_multipole, up_t, send_cells.reshape(devices, CAP_NEAR))),
    )
    low = shifted(up_send, 1)
    high = shifted(down_send, -1)
    far = lax.all_to_all(far_send, "leaf", split_axis=0, concat_axis=0, tiled=True)
    plus = shifted(rows([plus_own, low[EXTRA : 2 * EXTRA], high[2 * EXTRA : 3 * EXTRA]]), 3)
    minus = shifted(
        rows([minus_own, high[EXTRA : 2 * EXTRA], low[2 * EXTRA : 3 * EXTRA]]), -3
    )
    index_rows = (TYPES * cells // LANES + 7) // 8 * 8
    index, local_own, wd, path = pl.pallas_call(
        tree_kernel,
        out_shape=[
            kept((index_rows, LANES), jnp.int32),
            kept((cells, LANES), F32),
            kept((LANES, 2 * PAIR), BF16),
            kept((LANES, (devices.bit_length() - 1) * PAIR), BF16),
        ],
        in_specs=[SM, VM, VM, VM, VM],
        out_specs=[VM] * 4,
        scratch_shapes=[
            scratch((LANES, 2 * PAIR), BF16),
            scratch((4, LANES, LANES), F32),
        ],
        cost_estimate=cost(10**9),
        compiler_params=limits(16),
        name="tree",
    )(own, far_list, held(agg), down_t, sibling_t)
    near_part = pl.pallas_call(
        near_kernel,
        out_shape=kept((elems, cells), F32),
        in_specs=[SM] + [VM] * 5,
        out_specs=VM,
        scratch_shapes=[
            scratch((cells + LANES, elems), BF16),
            scratch((LANES, cells), F32),
        ],
        cost_estimate=cost(10**9),
        compiler_params=limits(16),
        name="near",
    )(own, held(slip_rows), held(low), held(high), near_list, held(near_blocks))
    table_rows = cells + devices * CAP_FAR + len(OFFSETS) * EXTRA
    return pl.pallas_call(
        leaf_kernel,
        out_shape=shape((elems, cells), F32),
        in_specs=[SM] + [VM] * 10 + [VM] * 4,
        out_specs=VM,
        scratch_shapes=[
            pltpu.SMEM((index_rows, LANES), jnp.int32),
            pltpu.SemaphoreType.DMA,
            scratch((table_rows, LANES), F32),
            scratch((2 * devices, LANES), F32),
            scratch((elems, LANES), BF16),
        ]
        + [scratch((cells, LANES), F32)] * 6,
        compiler_params=limits(24),
        name="leaf",
    )(
        own,
        held(index),
        held(far),
        held(low),
        held(high),
        held(plus),
        held(minus),
        held(mult),
        held(wu),
        held(wd),
        held(path),
        held(leaf_far),
        held(to_stress),
        held(local_own),
        held(near_part),
    )


def solution(mesh):
    return jax.shard_map(
        body,
        mesh=mesh,
        in_specs=(
            P(None, "leaf"),
            P(),
            P(),
            P(),
            P(),
            P(),
            P(),
            P(),
            P("leaf", None),
            P(None, "leaf"),
            P(None, "leaf"),
        ),
        out_specs=P(None, "leaf"),
        check_vma=False,
    )
```
